32 devices in a mesh: cfg: 2 (over x), seq: 16 (over z, y, core).
Axes of the slice: x: 2, y: 2, z: 4, core: 2. Of those that a mesh axis runs over, the one named last changes fastest.
Arguments:
- coarse_hidden: bfloat16 [2, 32, 64, 2048], P('cfg', 'seq'), may hold values from -6 to 6
- coarse_modulation: float32 [2, 2, 2048], P('cfg'), may hold values from -3 to 3
- final_weight: bfloat16 [2048, 32], replicated, may hold values from -0.125 to 0.125
- coarse_latent: float32 [32, 2048], P('seq'), may hold values from -6 to 6
- step_index: int32 [1], replicated, may hold values from 0 to 49
- guide_index: int32 [1], replicated, may hold values from 0 to 4095
- guide_scales: float32 [4096], replicated, may hold values from 1.5 to 6
- upsample_weight: float32 [288, 32], replicated, may hold values from -0.375 to 0.375
- upsample_bias: float32 [32], replicated, may hold values from -3 to 3
- embed_weight: bfloat16 [32, 2048], replicated, may hold values from -1 to 1
- embed_bias: float32 [2048], replicated, may hold values from -3 to 3
- fine_modulation: float32 [3, 2048], replicated, may hold values from -3 to 3
- project_weight: bfloat16 [2048, 3072], P(('cfg', 'seq')), may hold values from -0.125 to 0.125
- query_gain: float32 [128], replicated, may hold values from 0.25 to 1.75
- key_gain: float32 [128], replicated, may hold values from 0.25 to 1.75
- text_keys: bfloat16 [256, 1024], replicated, may hold values from -6 to 6
- text_values: bfloat16 [256, 1024], replicated, may hold values from -6 to 6
- text_length: int32 [1], replicated, may hold values from 192 to 256
- output_weight: bfloat16 [1024, 2048], P(None, ('cfg', 'seq')), may hold values from -0.1875 to 0.1875
Outputs:
- guided_velocity: float32 [32, 2048], P('seq')
- fine_latent: float32 [32, 2, 4096], P('seq', 'cfg')
- fine_hidden: bfloat16 [32, 2, 128, 2048], P('seq', 'cfg')
The draws below stay inside these ranges and needn't reach their ends.
All inputs are finite; a program needn't handle non-finite values.
Results may differ from the reference program's by a relative error of at most 0.0053.
Values may be sent and summed in bfloat16 or wider, within the bound.
No kernel may reach another device: no remote copies, remote signals or barrier semaphores. Data moves between devices by JAX's collectives and lax.ppermute only.
A program may use at most 128 MiB of HBM per device.

```python
import jax
import jax.numpy as jnp
from jax import lax

D = 2048
HEAD_DIM = 128
CHANNELS = 32
HEADS = 8
WA = 64
TEXT = 256
GUIDES = 4096
STEPS = 50
REACH = 1
HA = 32
INNER = 1024


def draw_fine_modulation(key, part):
    shift_key = jax.random.fold_in(key, 11)
    size_key = jax.random.fold_in(key, 12)
    sign_key = jax.random.fold_in(key, 13)
    leading = jnp.clip(0.5 * jax.random.normal(shift_key, (2, D), jnp.float32), -3.0, 3.0)
    magnitude = jax.random.uniform(size_key, (1, D), jnp.float32, 2.0, 3.0)
    signs = jnp.where(jax.random.bernoulli(sign_key, 0.5, (1, D)), 1.0, -1.0)
    return jnp.concatenate([leading, magnitude * signs], 0).astype(jnp.float32)


def levels(rng, extent, shards, smallest, top_value):
    def one(dim, parts):
        steps = jax.random.uniform(jax.random.fold_in(jax.random.fold_in(rng, 6), dim), (parts,), jnp.float32, smallest / len(shards), top_value / len(shards))
        return jnp.repeat(jnp.exp(steps), extent[dim] // parts).reshape((-1,) + (1,) * (len(extent) - dim - 1))

    factor_of = one(*shards[0])
    for cut in shards[1:]:
        factor_of = factor_of * one(*cut)
    return factor_of


def normal_values(rng, shape, scale, bound, cuts=(), kind=jnp.bfloat16):
    values = jax.random.normal(rng, shape, jnp.float32) * scale
    if len(cuts) > 0:
        values = levels(rng, shape, cuts, -0.22, 0.18) * values
    return jnp.clip(values, min=-bound, max=bound).astype(kind)


def setup_inputs(seed: int = 0) -> dict:
    seeds = jax.random.split(jax.random.key(seed), 20)
    coarse_hidden = normal_values(seeds[0], (2, HA, WA, D), 1.0, 6.0, ((0, 2), (1, 16)))
    coarse_modulation = normal_values(seeds[1], (2, 2, D), 0.5, 3.0, ((0, 2),), jnp.float32)
    final_weight = normal_values(seeds[2], (D, CHANNELS), D ** -0.5, 0.125)
    coarse_latent = normal_values(seeds[3], (HA, WA * CHANNELS), 1.0, 6.0, ((0, 16),), jnp.float32)
    step_index = jax.random.randint(seeds[4], (1,), 0, STEPS).astype(jnp.int32)
    guide_index = jax.random.randint(seeds[5], (1,), 0, GUIDES).astype(jnp.int32)
    guide_scales = jnp.clip(jax.random.uniform(seeds[6], (GUIDES,), jnp.float32, 1.5, 6.0), 1.5, 6.0)
    upsample_weight = normal_values(seeds[7], (9 * CHANNELS, CHANNELS), (9 * CHANNELS) ** -0.5, 0.375, (), jnp.float32)
    upsample_bias = normal_values(seeds[8], (CHANNELS,), 0.5, 3.0, (), jnp.float32)
    embed_weight = normal_values(seeds[9], (CHANNELS, D), CHANNELS ** -0.5, 1.0)
    embed_bias = normal_values(seeds[10], (D,), 0.5, 3.0, (), jnp.float32)
    fine_modulation = draw_fine_modulation(jax.random.fold_in(seeds[19], 71), 0)
    project_weight = normal_values(seeds[12], (D, 3 * INNER), D ** -0.5, 0.125, ((0, 32),))
    query_gain = jnp.clip(1.0 + 0.15 * jax.random.normal(seeds[13], (HEAD_DIM,), jnp.float32), 0.25, 1.75)
    key_gain = jnp.clip(1.0 + 0.15 * jax.random.normal(seeds[14], (HEAD_DIM,), jnp.float32), 0.25, 1.75)
    text_keys = normal_values(seeds[15], (TEXT, INNER), 1.0, 6.0)
    text_values = jnp.clip(jax.random.uniform(seeds[16], (TEXT, INNER), jnp.float32, -6.0, 6.0), -6.0, 6.0).astype(jnp.bfloat16)
    text_length = jax.random.randint(seeds[17], (1,), TEXT * 3 // 4, TEXT + 1).astype(jnp.int32)
    output_weight = normal_values(seeds[18], (INNER, D), INNER ** -0.5, 0.1875, ((1, 32),))
    return {"coarse_hidden": coarse_hidden, "coarse_modulation": coarse_modulation, "final_weight": final_weight, "coarse_latent": coarse_latent, "step_index": step_index, "guide_index": guide_index, "guide_scales": guide_scales, "upsample_weight": upsample_weight, "upsample_bias": upsample_bias, "embed_weight": embed_weight, "embed_bias": embed_bias, "fine_modulation": fine_modulation, "project_weight": project_weight, "query_gain": query_gain, "key_gain": key_gain, "text_keys": text_keys, "text_values": text_values, "text_length": text_length, "output_weight": output_weight}


epsilon = 1e-06
flow_shift = 5.0
highest = lax.Precision.HIGHEST

def layer_norm(values):
    centred = values - lax.optimization_barrier(jnp.mean(values, -1, keepdims=True))
    return centred * lax.rsqrt(lax.optimization_barrier(jnp.mean(centred * centred, -1, keepdims=True)) + epsilon)

def rms_heads(values, gain_vector, head_width):
    shaped = values.reshape(values.shape[0], -1, head_width)
    scaled = shaped * lax.rsqrt(lax.optimization_barrier(jnp.mean(shaped * shaped, -1, keepdims=True)) + epsilon) * gain_vector
    return scaled.reshape(values.shape[0], -1)

def sigma_at(step_value):
    fraction = 1.0 - step_value.astype(jnp.float32) / STEPS
    return flow_shift * fraction / (1.0 + (flow_shift - 1.0) * fraction)

def pick_scale(scale_table, slot_index):
    slots = jnp.arange(scale_table.shape[0], dtype=jnp.int32)
    return jnp.sum(jnp.where(slots == slot_index, scale_table, 0.0))

def attend(queries, image_keys, image_values, text_keys, text_values, image_mask, text_mask, heads):
    head_width = queries.shape[1] // heads
    score_scale = head_width ** (-0.5)
    dims = (((1,), (1,)), ((), ()))

    def one_head(head_index):
        column_start = head_index * head_width
        query_part = lax.dynamic_slice_in_dim(queries, column_start, head_width, 1)
        key_part = lax.dynamic_slice_in_dim(image_keys, column_start, head_width, 1)
        value_part = lax.dynamic_slice_in_dim(image_values, column_start, head_width, 1)
        text_key_part = lax.dynamic_slice_in_dim(text_keys, column_start, head_width, 1)
        text_value_part = lax.dynamic_slice_in_dim(text_values, column_start, head_width, 1)
        image_scores = lax.dot_general(query_part, key_part, dims, preferred_element_type=jnp.float32) * score_scale
        text_scores = lax.dot_general(query_part, text_key_part, dims, preferred_element_type=jnp.float32) * score_scale
        image_weights = jnp.where(image_mask, jnp.exp(image_scores), 0.0)
        text_weights = jnp.where(text_mask, jnp.exp(text_scores), 0.0)
        denominator = lax.optimization_barrier(jnp.sum(image_weights, 1, keepdims=True)) + lax.optimization_barrier(jnp.sum(text_weights, 1, keepdims=True))
        image_weights = (image_weights / denominator).astype(jnp.bfloat16)
        text_weights = (text_weights / denominator).astype(jnp.bfloat16)
        return jnp.dot(image_weights, value_part, preferred_element_type=jnp.float32) + jnp.dot(text_weights, text_value_part, preferred_element_type=jnp.float32)
    stacked = lax.map(one_head, jnp.arange(heads, dtype=jnp.int32))
    return stacked.transpose(1, 0, 2).reshape(queries.shape[0], -1).astype(jnp.bfloat16)

def upsample_conv(latent_grid, upsample_weight, upsample_bias):
    upsampled = jnp.repeat(jnp.repeat(latent_grid, 2, 0), 2, 1)
    padded = jnp.pad(upsampled, ((1, 1), (1, 1), (0, 0)))
    height, breadth = (upsampled.shape[0], upsampled.shape[1])
    tap_list = [padded[row_shift:row_shift + height, col_shift:col_shift + breadth] for row_shift in range(3) for col_shift in range(3)]
    patches = jnp.concatenate(tap_list, -1).reshape(height * breadth, -1)
    product = jnp.dot(patches, upsample_weight, precision=highest).reshape(height, breadth, -1)
    return product + upsample_bias + upsampled

def reference(coarse_hidden, coarse_modulation, final_weight, coarse_latent, step_index, guide_index, guide_scales, upsample_weight, upsample_bias, embed_weight, embed_bias, fine_modulation, project_weight, query_gain, key_gain, text_keys, text_values, text_length, output_weight):
    velocities = []
    for branch in range(2):
        normed = layer_norm(coarse_hidden[branch].astype(jnp.float32))
        modulated = (normed * (1.0 + coarse_modulation[branch, 1]) + coarse_modulation[branch, 0]).astype(jnp.bfloat16)
        flat_velocity = jnp.dot(modulated.reshape(-1, D), final_weight, preferred_element_type=jnp.float32)
        velocities.append(flat_velocity.reshape(HA, WA * CHANNELS))
    guidance = pick_scale(guide_scales, guide_index[0])
    guided = velocities[1] + guidance * (velocities[0] - velocities[1])
    stepped = coarse_latent + (sigma_at(step_index[0] + 1) - sigma_at(step_index[0])) * guided
    fine_full = upsample_conv(stepped.reshape(HA, WA, CHANNELS), upsample_weight, upsample_bias)
    fine_latent = fine_full.reshape(HA, 2, 2 * WA * CHANNELS)
    fine_tokens = fine_full.reshape(HA, 4 * WA, CHANNELS)
    normed_text_keys = rms_heads(text_keys.astype(jnp.float32), key_gain, HEAD_DIM).astype(jnp.bfloat16)

    def state_row(tokens):
        fine_state = jnp.dot(tokens.astype(jnp.bfloat16), embed_weight, preferred_element_type=jnp.float32) + embed_bias
        fine_normed = (layer_norm(fine_state) * (1.0 + fine_modulation[1]) + fine_modulation[0]).astype(jnp.bfloat16)
        return (fine_state, fine_normed)

    def project_row(tokens):
        fine_normed = state_row(tokens)[1]
        projected = jnp.dot(fine_normed, project_weight, preferred_element_type=jnp.float32)
        queries = rms_heads(projected[:, :INNER], query_gain, HEAD_DIM).astype(jnp.bfloat16)
        keys = rms_heads(projected[:, INNER:2 * INNER], key_gain, HEAD_DIM).astype(jnp.bfloat16)
        values = projected[:, 2 * INNER:].astype(jnp.bfloat16)
        return (queries, keys, values)
    all_queries, all_keys, all_values = lax.map(project_row, fine_tokens)
    padded_keys = jnp.pad(all_keys, ((REACH, REACH), (0, 0), (0, 0)))
    padded_values = jnp.pad(all_values, ((REACH, REACH), (0, 0), (0, 0)))
    text_mask = (jnp.arange(TEXT, dtype=jnp.int32) < text_length[0])[None, :]
    key_offsets = jnp.arange((2 * REACH + 1) * 4 * WA, dtype=jnp.int32) // (4 * WA)

    def attend_row(row_index):
        window_keys = lax.dynamic_slice_in_dim(padded_keys, row_index, 2 * REACH + 1, 0).reshape(-1, INNER)
        window_values = lax.dynamic_slice_in_dim(padded_values, row_index, 2 * REACH + 1, 0).reshape(-1, INNER)
        global_rows = row_index - REACH + key_offsets
        valid = (global_rows >= 0) & (global_rows < HA)
        image_mask = jnp.broadcast_to(valid[None, :], (4 * WA, valid.shape[0]))
        queries = lax.dynamic_index_in_dim(all_queries, row_index, 0, keepdims=False)
        attended = attend(queries, window_keys, window_values, normed_text_keys, text_values, image_mask, text_mask, HEADS)
        fine_state = state_row(lax.dynamic_index_in_dim(fine_tokens, row_index, 0, keepdims=False))[0]
        output_part = jnp.dot(attended, output_weight, preferred_element_type=jnp.float32)
        return (fine_state + fine_modulation[2] * output_part).astype(jnp.bfloat16).reshape(2, 2 * WA, D)
    fine_hidden = lax.map(attend_row, jnp.arange(HA, dtype=jnp.int32))
    return (guided, fine_latent, fine_hidden)
```

```python
import functools

import jax
import jax.numpy as jnp
from jax import lax
from jax.experimental import pallas as pl
from jax.experimental.pallas import tpu as pltpu
from jax.sharding import PartitionSpec as P

HEADS = 8
STEPS = 50

epsilon = 1e-06
flow_shift = 5.0
highest = lax.Precision.HIGHEST
f32 = jnp.float32
bf16 = jnp.bfloat16
LOG2E = 1.4426950408889634
TERMS = 40
SLAB = 48
DEPTH = 256


def vmem(count):
    return [pl.BlockSpec(memory_space=pltpu.VMEM) for _ in range(count)]


def smem(count):
    return [pl.BlockSpec(memory_space=pltpu.SMEM) for _ in range(count)]


def cost(flops, moved):
    return pl.CostEstimate(flops=int(flops), bytes_accessed=int(moved), transcendentals=0)


def dot_rows(left, right):
    return lax.dot_general(left, right, (((0,), (0,)), ((), ())), preferred_element_type=f32)


def split(values):
    high = values.astype(bf16)
    return high, (values - high.astype(f32)).astype(bf16)


def centred_embedding(embed, bias):
    width = embed.shape[1]
    embed = embed - jnp.sum(embed, -1, keepdims=True) * (1.0 / width)
    bias = bias - jnp.sum(bias, -1, keepdims=True) * (1.0 / width)
    return embed, bias


def with_tail(body, first, second):
    row = lax.broadcasted_iota(jnp.int32, (16, body.shape[1]), 0)
    tail = jnp.where(row == 0, first, jnp.where(row == 1, second, 0.0))
    return jnp.concatenate([body, tail], 0)


def partial_kernel(seq_count, embed_ref, bias_ref, mod_ref, weight_ref, keep_ref, send_ref):
    seq_index = lax.axis_index("seq")
    core = seq_index % 2
    depth = weight_ref.shape[0]
    half = keep_ref.shape[1]
    embed = embed_ref[...].astype(f32)
    width = embed.shape[1]
    embed_mean = jnp.sum(embed, -1, keepdims=True) * (1.0 / width)
    bias_mean = jnp.sum(bias_ref[...], -1, keepdims=True) * (1.0 / width)
    start = (lax.axis_index("cfg") * seq_count + seq_index) * depth
    base = pl.multiple_of(start // 128 * 128, 128)
    offset = start - base
    window = pl.ds(base, 128)
    scale = 1.0 + mod_ref[1:2, window]
    rows = with_tail(
        (embed_ref[:, window].astype(f32) - embed_mean) * scale,
        (bias_ref[:, window] - bias_mean) * scale,
        mod_ref[0:1, window],
    )
    rows = pltpu.roll(rows, (128 - offset) % 128, 1)[:, :depth]
    high, low = split(rows)
    left = jnp.concatenate([high, low], 0)

    def part(which):
        columns = pl.ds(pl.multiple_of(which * half, 128), half)
        product = jnp.dot(left, weight_ref[:, columns], preferred_element_type=f32)
        return product[:TERMS] + product[SLAB : SLAB + TERMS]

    send_ref[...] = part(1 - core).astype(bf16)
    keep_ref[...] = part(core)


def velocity_kernel(hidden_ref, mod_ref, weight_ref, out_ref):
    values = hidden_ref[...].astype(f32)
    width = values.shape[1]
    centred = values - jnp.sum(values, -1, keepdims=True) * (1.0 / width)
    variance = jnp.sum(centred * centred, -1, keepdims=True) * (1.0 / width)
    normed = centred * lax.rsqrt(variance + epsilon)
    modulated = (normed * (1.0 + mod_ref[1:2, :]) + mod_ref[0:1, :]).astype(bf16)
    out_ref[...] = jnp.dot(modulated, weight_ref[...], preferred_element_type=f32).T


def guide_kernel(step_ref, slot_ref, table_ref, own_ref, other_ref, latent_ref, guided_ref, next_ref):
    branch = lax.axis_index("cfg")
    own = own_ref[...]
    other = other_ref[...]
    first = branch == 0
    conditional = jnp.where(first, own, other)
    unconditional = jnp.where(first, other, own)
    table = table_ref[...]
    slots = lax.broadcasted_iota(jnp.int32, table.shape, 0) * table.shape[
        1
    ] + lax.broadcasted_iota(jnp.int32, table.shape, 1)
    picked = jnp.where(slots == slot_ref[0], table, 0.0)
    guidance = jnp.sum(jnp.sum(picked, 0, keepdims=True), 1, keepdims=True)
    guided = unconditional + guidance * (conditional - unconditional)

    def sigma(step):
        fraction = 1.0 - jnp.full((1, 128), step, jnp.int32).astype(f32) / STEPS
        return flow_shift * fraction / (1.0 + (flow_shift - 1.0) * fraction)

    change = (sigma(step_ref[0] + 1) - sigma(step_ref[0]))[:, :1]
    guided_ref[...] = guided
    next_ref[...] = latent_ref[...] + change * guided


def fine_kernel(
    cells,
    up_ref,
    own_ref,
    down_ref,
    taps_ref,
    shift_ref,
    embed_ref,
    bias_ref,
    text_ref,
    gain_ref,
    fine_ref,
    keys_ref,
    keys_t_ref,
    query_ref,
    token_ref,
    text_out_ref,
):
    channels, own_lanes = own_ref.shape
    rows = own_lanes // cells
    lanes = (rows + 2) * cells
    gain = gain_ref[...]
    head = gain.shape[1]
    for h in range(text_ref.shape[1] // head):
        part = text_ref[:, h * head : (h + 1) * head].astype(f32)
        mean = jnp.sum(part * part, -1, keepdims=True) * (1.0 / head)
        text_out_ref[:, h * head : (h + 1) * head] = (
            part * lax.rsqrt(mean + epsilon) * gain
        ).astype(bf16)

    extended = jnp.concatenate([up_ref[...], own_ref[...], down_ref[...]], 1)
    total = extended.shape[1]
    origin = own_lanes - cells
    lane = lax.broadcasted_iota(jnp.int32, (channels, lanes), 1) % cells

    def shifted(down, right):
        start = origin + down * cells + right
        moved = pltpu.roll(extended, (-start) % total, 1)[:, :lanes]
        if right < 0:
            moved = jnp.where(lane == 0, 0.0, moved)
        if right > 0:
            moved = jnp.where(lane == cells - 1, 0.0, moved)
        return moved

    around = {(i, j): shifted(i, j) for i in (-1, 0, 1) for j in (-1, 0, 1)}

    def tap(r, s):
        first = (3 * r + s) * channels
        return taps_ref[first : first + channels, :]

    blocks = {}
    for a in range(2):
        for c in range(2):
            patches, weights = [], []
            for i in (a - 1, a):
                for j in (c - 1, c):
                    merged = None
                    for r in range(3):
                        for s in range(3):
                            if (a + r - 1) // 2 == i and (c + s - 1) // 2 == j:
                                merged = tap(r, s) if merged is None else merged + tap(r, s)
                    patches.append(around[i, j])
                    weights.append(merged)
            stacked = jnp.concatenate(weights, 0).T
            product = jnp.dot(
                stacked, jnp.concatenate(patches, 0), precision=highest, preferred_element_type=f32
            )
            blocks[a, c] = product + shift_ref[...] + around[0, 0]

    embed, bias = centred_embedding(embed_ref[...].astype(f32), bias_ref[...])
    high, low = split(with_tail(embed, bias, jnp.zeros_like(bias)))
    pair = jnp.concatenate([high, low], 0)
    width = embed.shape[1]
    step = min(width, 512)

    def features(tokens):
        count = tokens.shape[1]
        one = jnp.ones((1, count), f32)
        values = with_tail(tokens.astype(f32), one, jnp.zeros_like(one)).astype(bf16)
        double = jnp.concatenate([values, values], 0)
        square = jnp.zeros((1, count), f32)
        for first in range(0, width, step):
            state = dot_rows(pair[:, first : first + step], double)
            square += jnp.sum(state * state, 0, keepdims=True)
        spread = lax.rsqrt(square * (1.0 / width) + epsilon)
        top, rest = split(with_tail(tokens.astype(f32) * spread, spread, one))
        fill = jnp.zeros((DEPTH - 3 * SLAB, count), bf16)
        return jnp.concatenate([top, rest, top, fill], 0)

    for a in range(2):
        for c in range(2):
            turned = features(blocks[a, c].astype(bf16)).T
            for r in range(rows + 2):
                first = (4 * r + 2 * a + c) * cells
                keys_ref[first : first + cells, :] = turned[r * cells : (r + 1) * cells, :]
    keys_t_ref[...] = keys_ref[...].T

    parity = lax.axis_index("cfg")
    tokens = jnp.zeros((channels, 2 * own_lanes), f32)
    cell = lax.broadcasted_iota(jnp.int32, (own_lanes, 2 * own_lanes), 0)
    place = lax.broadcasted_iota(jnp.int32, (own_lanes, 2 * own_lanes), 1)
    for c in range(2):
        mine = jnp.where(parity == 0, blocks[0, c], blocks[1, c])
        mine = pltpu.roll(mine, lanes - cells, 1)[:, :own_lanes]
        fine_ref[c] = mine
        chosen = jnp.where(place == 2 * cell + c, 1.0, 0.0).astype(bf16)
        tokens += jnp.dot(mine.astype(bf16), chosen, preferred_element_type=f32)
    token_ref[...] = tokens.astype(bf16)
    query_ref[...] = features(tokens.astype(bf16)).T


def attend_kernel(
    rows,
    window,
    length_ref,
    kept_ref,
    other_ref,
    keys_ref,
    keys_t_ref,
    query_ref,
    query_gain_ref,
    key_gain_ref,
    text_ref,
    text_values_ref,
    out_ref,
    mix_ref,
    value_ref,
):
    head_index = pl.program_id(0)
    heads = pl.num_programs(0)
    seq_index = lax.axis_index("seq")
    head = query_gain_ref.shape[1]
    half = kept_ref.shape[1]
    key_count = keys_ref.shape[0]
    text_count = text_ref.shape[0]
    inner = heads * head
    low_ok = seq_index > 0
    high_ok = seq_index < lax.axis_size("seq") - 1
    key_row = lax.broadcasted_iota(jnp.int32, (key_count, head), 0)
    allowed = (low_ok | (key_row >= window)) & (high_ok | (key_row < key_count - window))
    text_row = lax.broadcasted_iota(jnp.int32, (text_count, head), 0)
    text_allowed = text_row < length_ref[0]

    @pl.when(head_index == 0)
    def _():
        core = seq_index % 2
        mix_ref[...] = jnp.zeros_like(mix_ref)
        kept = kept_ref[...]
        top, rest = split(kept)
        mine = pl.ds(pl.multiple_of(core * half, 128), half)
        mix_ref[0:TERMS, mine] = top
        mix_ref[SLAB : SLAB + TERMS, mine] = top
        mix_ref[2 * SLAB : 2 * SLAB + TERMS, mine] = rest
        theirs = pl.ds(pl.multiple_of((1 - core) * half, 128), half)
        mix_ref[0:TERMS, theirs] = other_ref[...]
        mix_ref[SLAB : SLAB + TERMS, theirs] = other_ref[...]
        value_ref[0:key_count, head : 2 * head] = jnp.where(allowed, 1.0, 0.0).astype(bf16)
        value_ref[key_count : key_count + text_count, head : 2 * head] = jnp.where(
            text_allowed, 1.0, 0.0
        ).astype(bf16)

    def columns(which):
        return pl.ds(pl.multiple_of(which * inner + head_index * head, 128), head)

    query = jnp.dot(query_ref[...], mix_ref[:, columns(0)], preferred_element_type=f32)
    mean = jnp.sum(query * query, -1, keepdims=True) * (1.0 / head)
    query = (query * lax.rsqrt(mean + epsilon) * query_gain_ref[...]).astype(bf16)
    keys = dot_rows(mix_ref[:, columns(1)], keys_t_ref[...])
    mean = jnp.sum(keys * keys, 0, keepdims=True) * (1.0 / head)
    keys = (keys * lax.rsqrt(mean + epsilon) * key_gain_ref[...]).astype(bf16)
    values = jnp.dot(keys_ref[...], mix_ref[:, columns(2)], preferred_element_type=f32)
    value_ref[0:key_count, 0:head] = jnp.where(allowed, values, 0.0).astype(bf16)
    value_ref[key_count : key_count + text_count, 0:head] = jnp.where(
        text_allowed, text_values_ref[...].astype(f32), 0.0
    ).astype(bf16)
    factor = head ** (-0.5) * LOG2E
    tokens = query.shape[0] // rows
    for r in range(rows):
        part = query[r * tokens : (r + 1) * tokens]
        near = slice(r * window, (r + 3) * window)
        scores = jnp.dot(part, keys[:, near], preferred_element_type=f32)
        text_scores = lax.dot_general(
            part, text_ref[...], (((1,), (1,)), ((), ())), preferred_element_type=f32
        )
        mixed = jnp.dot(
            jnp.exp2(scores * factor).astype(bf16), value_ref[near, :], preferred_element_type=f32
        ) + jnp.dot(
            jnp.exp2(text_scores * factor).astype(bf16),
            value_ref[key_count : key_count + text_count, :],
            preferred_element_type=f32,
        )
        out_ref[r * tokens : (r + 1) * tokens, :] = (mixed[:, :head] / mixed[:, head:]).astype(bf16)


def output_kernel(
    orders,
    attended_ref,
    token_ref,
    embed_ref,
    bias_ref,
    gate_ref,
    own_a_ref,
    own_b_ref,
    other_a_ref,
    other_b_ref,
    out_ref,
):
    chips, piece, inner = own_a_ref.shape
    seq_index = lax.axis_index("seq")
    core = seq_index % 2
    coordinate = {"cfg": lax.axis_index("cfg"), "seq": seq_index // 2}
    seq_chips = lax.axis_size("seq") // 2
    attended = attended_ref[...]
    tokens = token_ref[...]

    def place(chip, order):
        target = {"cfg": chip // seq_chips, "seq": chip % seq_chips}
        position = 0
        for level, (axis, bit) in enumerate(order):
            shift = bit - 1 if axis == "seq" else bit
            differs = ((coordinate[axis] >> shift) & 1) ^ ((target[axis] >> shift) & 1)
            position = position + (differs << level)
        return position

    for chip in range(chips):
        at_a, at_b = place(chip, orders[0]), place(chip, orders[1])
        weight = jnp.concatenate(
            [own_a_ref[at_a], own_b_ref[at_b], other_a_ref[at_a], other_b_ref[at_b]], 0
        )
        product = lax.dot_general(
            attended, weight, (((1,), (1,)), ((), ())), preferred_element_type=f32
        )
        product = pltpu.roll(product, core * 2 * piece, 1)
        lanes = slice(chip * 4 * piece, (chip + 1) * 4 * piece)
        state = dot_rows(tokens, embed_ref[:, lanes]) + bias_ref[:, lanes]
        out_ref[:, lanes] = (state + gate_ref[:, lanes] * product).astype(bf16)


def per_device(
    coarse_hidden,
    coarse_modulation,
    final_weight,
    coarse_latent,
    step_index,
    guide_index,
    guide_scales,
    upsample_weight,
    upsample_bias,
    embed_weight,
    embed_bias,
    fine_modulation,
    project_weight,
    query_gain,
    key_gain,
    text_keys,
    text_values,
    text_length,
    output_weight,
):
    rows = coarse_hidden.shape[1]
    cells = coarse_hidden.shape[2]
    width = coarse_hidden.shape[3]
    channels = final_weight.shape[1]
    head = query_gain.shape[0]
    inner = project_weight.shape[1] // 3
    cfg_count = lax.axis_size("cfg")
    seq_count = lax.axis_size("seq")
    seq_index = lax.axis_index("seq")
    seq_bits = seq_count.bit_length() - 1
    assert seq_count == 1 << seq_bits and cfg_count == 2 and rows >= 2
    own = rows * cells
    fine_tokens = 2 * own
    key_count = (rows + 2) * 4 * cells
    text_count = text_keys.shape[0]
    bias_row = embed_bias.reshape(1, width)

    def swap(value, *stages):
        size = cfg_count * seq_count
        flip = 0
        for axis, bit in stages:
            flip |= seq_count if axis == "cfg" else 1 << bit
        return lax.ppermute(value, ("cfg", "seq"), [(i, i ^ flip) for i in range(size)])

    across = ("seq", 0)
    levels = [("cfg", 0)] + [("seq", bit) for bit in range(1, seq_bits)]

    half = 3 * inner // 2
    kept, sent = pl.pallas_call(
        functools.partial(partial_kernel, seq_count),
        out_shape=(
            jax.ShapeDtypeStruct((TERMS, half), f32),
            jax.ShapeDtypeStruct((TERMS, half), bf16),
        ),
        in_specs=vmem(4),
        out_specs=tuple(vmem(2)),
        cost_estimate=cost(2 * 96 * 64 * 3 * inner, 1e6),
        name="partial_mix",
    )(embed_weight, bias_row, fine_modulation, project_weight)

    velocity = pl.pallas_call(
        velocity_kernel,
        out_shape=jax.ShapeDtypeStruct((channels, own), f32),
        in_specs=vmem(3),
        out_specs=vmem(1)[0],
        cost_estimate=cost(2 * own * width * 128, 1e6),
        name="velocity",
    )(coarse_hidden.reshape(own, width), coarse_modulation[0], final_weight)

    total = kept + swap(sent, across).astype(f32)
    partner = swap(velocity, ("cfg", 0))

    piece = output_weight.shape[1] // 2
    turned = output_weight.T
    orders = (tuple(levels), tuple(levels[2:] + levels[:2]))

    def gathered(block, order):
        held = block[None]
        for stage in order:
            held = jnp.concatenate([held, swap(held, stage)], 0)
        return held

    first, second = levels[0], levels[1]
    rounded = total.astype(bf16)
    total = (
        total
        + swap(rounded, first).astype(f32)
        + swap(rounded, second).astype(f32)
        + swap(rounded, first, second).astype(f32)
    )
    for stage in levels[2:]:
        total = total + swap(total.astype(bf16), stage).astype(f32)
    others = swap(total.astype(bf16), across)

    latent = coarse_latent.reshape(own, channels).T
    guided, stepped = pl.pallas_call(
        guide_kernel,
        out_shape=(jax.ShapeDtypeStruct((channels, own), f32),) * 2,
        in_specs=smem(2) + vmem(4),
        out_specs=tuple(vmem(2)),
        cost_estimate=cost(1e6, 1e5),
        name="guide",
    )(step_index, guide_index, guide_scales.reshape(-1, 128), velocity, partner, latent)

    forward = [(i, i + 1) for i in range(seq_count - 1)]
    backward = [(target, source) for source, target in forward]
    up = lax.ppermute(stepped, "seq", forward)
    down = lax.ppermute(stepped, "seq", backward)

    fine, keys, keys_t, query, tokens, text_normed = pl.pallas_call(
        functools.partial(fine_kernel, cells),
        out_shape=(
            jax.ShapeDtypeStruct((2, channels, own), f32),
            jax.ShapeDtypeStruct((key_count, DEPTH), bf16),
            jax.ShapeDtypeStruct((DEPTH, key_count), bf16),
            jax.ShapeDtypeStruct((fine_tokens, DEPTH), bf16),
            jax.ShapeDtypeStruct((channels, fine_tokens), bf16),
            jax.ShapeDtypeStruct(text_keys.shape, bf16),
        ),
        in_specs=vmem(9),
        out_specs=tuple(vmem(6)),
        cost_estimate=cost(4e9, 4e6),
        name="fine_features",
    )(
        up,
        stepped,
        down,
        upsample_weight,
        upsample_bias.reshape(channels, 1),
        embed_weight,
        bias_row,
        text_keys,
        key_gain.reshape(1, head),
    )

    whole = pl.BlockSpec(memory_space=pltpu.VMEM)
    per_head = pl.BlockSpec((text_count, head), lambda h: (0, h))
    attended = pl.pallas_call(
        functools.partial(attend_kernel, rows, 4 * cells),
        grid=(HEADS,),
        out_shape=jax.ShapeDtypeStruct((fine_tokens, inner), bf16),
        in_specs=smem(1) + [whole] * 7 + [per_head, per_head],
        out_specs=pl.BlockSpec((fine_tokens, head), lambda h: (0, h)),
        scratch_shapes=[
            pltpu.VMEM((DEPTH, 3 * inner), bf16),
            pltpu.VMEM((key_count + text_count, 2 * head), bf16),
        ],
        cost_estimate=cost(8e9, 4e6),
        name="attend",
    )(
        text_length,
        total,
        others,
        keys,
        keys_t,
        query,
        query_gain.reshape(1, head),
        key_gain.reshape(head, 1),
        text_normed,
        text_values,
    )

    own_a = gathered(turned[:piece], orders[0])
    own_b = gathered(turned[piece:], orders[1])
    other_a = swap(own_a, across)
    other_b = swap(own_b, across)
    gate = fine_modulation[2:3]
    if piece % 16 == 0:
        hidden = pl.pallas_call(
            functools.partial(output_kernel, orders),
            out_shape=jax.ShapeDtypeStruct((fine_tokens, width), bf16),
            in_specs=vmem(9),
            out_specs=vmem(1)[0],
            cost_estimate=cost(2e9, 6e6),
            name="output",
        )(attended, tokens, embed_weight, bias_row, gate, own_a, own_b, other_a, other_b)
    else:
        chip = jnp.arange(cfg_count * seq_count // 2, dtype=jnp.int32)
        seq_chips = seq_count // 2
        apart = {
            "cfg": chip // seq_chips ^ lax.axis_index("cfg"),
            "seq": chip % seq_chips ^ seq_index // 2,
        }

        def ordered(block, order):
            position = jnp.zeros_like(chip)
            for level, (axis, bit) in enumerate(order):
                shift = bit - 1 if axis == "seq" else bit
                position = position + ((apart[axis] >> shift & 1) << level)
            return jnp.take(block, position, axis=0)

        mine = jnp.concatenate([ordered(own_a, orders[0]), ordered(own_b, orders[1])], 1)
        theirs = jnp.concatenate([ordered(other_a, orders[0]), ordered(other_b, orders[1])], 1)
        even = seq_index % 2 == 0
        both = jnp.stack([jnp.where(even, mine, theirs), jnp.where(even, theirs, mine)], 1)
        weight = both.reshape(width, inner)
        product = lax.dot_general(
            attended, weight, (((1,), (1,)), ((), ())), preferred_element_type=f32
        )
        state = dot_rows(tokens, embed_weight) + bias_row
        hidden = (state + gate * product).astype(bf16)

    fine_latent = fine.transpose(2, 0, 1).reshape(rows, 1, 2 * cells * channels)
    return (
        guided.T.reshape(rows, cells * channels),
        fine_latent,
        hidden.reshape(rows, 1, 2 * cells, width),
    )


def solution(mesh):
    placed = (
        P("cfg", "seq", None, None),
        P("cfg", None, None),
        P(),
        P("seq", None),
        P(),
        P(),
        P(),
        P(),
        P(),
        P(),
        P(),
        P(),
        P(("cfg", "seq"), None),
        P(),
        P(),
        P(),
        P(),
        P(),
        P(None, ("cfg", "seq")),
    )
    return jax.shard_map(
        per_device,
        mesh=mesh,
        in_specs=placed,
        out_specs=(P("seq", None), P("seq", "cfg", None), P("seq", "cfg", None, None)),
        check_vma=False,
    )
```

```python
import functools

import jax
import jax.numpy as jnp
from jax import lax
from jax.experimental import pallas as pl
from jax.experimental.pallas import tpu as pltpu
from jax.sharding import PartitionSpec as P

STEPS = 50

epsilon = 1e-06
flow_shift = 5.0
highest = lax.Precision.HIGHEST
f32 = jnp.float32
bf16 = jnp.bfloat16
LOG2E = 1.4426950408889634
TERMS = 40
SLAB = 48
DEPTH = 256


def vmem(count):
    return [pl.BlockSpec(memory_space=pltpu.VMEM) for _ in range(count)]


def cost(flops, moved):
    return pl.CostEstimate(flops=int(flops), bytes_accessed=int(moved), transcendentals=0)


def dot_rows(left, right):
    return lax.dot_general(left, right, (((0,), (0,)), ((), ())), preferred_element_type=f32)


def anywhere(count):
    return [pl.BlockSpec(memory_space=pl.ANY) for _ in range(count)]


def fetch(pairs, sems):
    copies = [pltpu.make_async_copy(src, dst, sems.at[i]) for i, (src, dst) in enumerate(pairs)]
    for copy in copies:
        copy.start()
    for copy in copies:
        copy.wait()


def exact(left, right, contract):
    return lax.dot_general(
        left, right, ((contract[:1], contract[1:]), ((), ())), precision=highest,
        preferred_element_type=f32,
    )


def lane_repeat(channels):
    lane = lax.broadcasted_iota(jnp.int32, (channels, 128), 1)
    row = lax.broadcasted_iota(jnp.int32, (channels, 128), 0)
    return jnp.where(lane % channels == row, 1.0, 0.0)


def split(values):
    high = values.astype(bf16)
    return high, (values - high.astype(f32)).astype(bf16)


def centred_embedding(embed, bias):
    width = embed.shape[1]
    embed = embed - jnp.sum(embed, -1, keepdims=True) * (1.0 / width)
    bias = bias - jnp.sum(bias, -1, keepdims=True) * (1.0 / width)
    return embed, bias


def with_tail(body, first, second):
    row = lax.broadcasted_iota(jnp.int32, (16, body.shape[1]), 0)
    tail = jnp.where(row == 0, first, jnp.where(row == 1, second, 0.0))
    return jnp.concatenate([body, tail], 0)


def partial_kernel(seq_count, embed_ref, bias_ref, mod_ref, weight_ref, keep_ref, send_ref):
    seq_index = lax.axis_index("seq")
    core = seq_index % 2
    depth = weight_ref.shape[0]
    half = keep_ref.shape[1]
    embed = embed_ref[...].astype(f32)
    width = embed.shape[1]
    embed_mean = jnp.sum(embed, -1, keepdims=True) * (1.0 / width)
    bias_mean = jnp.sum(bias_ref[...], -1, keepdims=True) * (1.0 / width)
    start = (lax.axis_index("cfg") * seq_count + seq_index) * depth
    base = pl.multiple_of(start // 128 * 128, 128)
    offset = start - base
    window = pl.ds(base, 128)
    scale = 1.0 + mod_ref[1:2, window]
    rows = with_tail(
        (embed_ref[:, window].astype(f32) - embed_mean) * scale,
        (bias_ref[:, window] - bias_mean) * scale,
        mod_ref[0:1, window],
    )
    rows = pltpu.roll(rows, (128 - offset) % 128, 1)[:, :depth]
    high, low = split(rows)
    left = jnp.concatenate([high, low], 0)

    def part(which):
        columns = pl.ds(pl.multiple_of(which * half, 128), half)
        product = jnp.dot(left, weight_ref[:, columns], preferred_element_type=f32)
        return product[:TERMS] + product[SLAB : SLAB + TERMS]

    send_ref[...] = part(1 - core)
    keep_ref[...] = part(core)


def velocity_kernel(hidden_ref, mod_ref, weight_ref, out_ref):
    values = hidden_ref[...].astype(f32)
    width = values.shape[1]
    centred = values - jnp.sum(values, -1, keepdims=True) * (1.0 / width)
    variance = jnp.sum(centred * centred, -1, keepdims=True) * (1.0 / width)
    normed = centred * lax.rsqrt(variance + epsilon)
    modulated = (normed * (1.0 + mod_ref[1:2, :]) + mod_ref[0:1, :]).astype(bf16)
    out_ref[...] = lax.dot_general(
        weight_ref[...], modulated, (((1,), (1,)), ((), ())), preferred_element_type=f32
    )


def guide_kernel(
    rows, step_ref, slot_ref, table_ref, latent_ref, own_any, other_any, guided_ref, next_ref,
    own_ref, other_ref, sems,
):
    fetch([(own_any, own_ref), (other_any, other_ref)], sems)
    branch = lax.axis_index("cfg")
    own = own_ref[...]
    other = other_ref[...]
    channels, count = own.shape
    group = 128 // channels
    cells = count // rows
    line = lax.broadcasted_iota(jnp.int32, (count // group, count), 0)
    column = lax.broadcasted_iota(jnp.int32, (count // group, count), 1)
    belongs = jnp.where(line == column % cells // group * rows + column // cells, 1.0, 0.0)
    lane = lax.broadcasted_iota(jnp.int32, (count, 128), 1)
    cell = lax.broadcasted_iota(jnp.int32, (count, 128), 0)
    slot = lane // channels == cell % group
    repeat = lane_repeat(channels)
    spread = jnp.where(slot, exact(belongs, latent_ref[...], (0, 0)), 0.0)
    latent = exact(repeat, spread, (1, 1))
    first = branch == 0
    conditional = jnp.where(first, own, other)
    unconditional = jnp.where(first, other, own)
    table = table_ref[...]
    slots = lax.broadcasted_iota(jnp.int32, table.shape, 0) * table.shape[
        1
    ] + lax.broadcasted_iota(jnp.int32, table.shape, 1)
    picked = jnp.where(slots == slot_ref[...], table, 0.0)
    guidance = jnp.sum(jnp.sum(picked, 0, keepdims=True), 1, keepdims=True)
    guided = unconditional + guidance * (conditional - unconditional)

    def sigma(step):
        fraction = 1.0 - step.astype(f32) / STEPS
        return flow_shift * fraction / (1.0 + (flow_shift - 1.0) * fraction)

    change = sigma(step_ref[...] + 1) - sigma(step_ref[...])
    next_ref[...] = latent + change * guided
    guided_ref[...] = exact(belongs, jnp.where(slot, exact(guided, repeat, (0, 0)), 0.0), (1, 0))


def fine_kernel(
    cells,
    taps_ref,
    shift_ref,
    embed_ref,
    bias_ref,
    text_ref,
    gain_ref,
    near_any,
    own_any,
    far_any,
    fine_ref,
    keys_ref,
    keys_t_ref,
    query_ref,
    token_ref,
    text_out_ref,
    near_ref,
    own_ref,
    far_ref,
    sems,
):
    fetch([(near_any, near_ref), (own_any, own_ref), (far_any, far_ref)], sems)
    channels, own_lanes = own_ref.shape
    rows = own_lanes // cells
    lanes = (rows + 2) * cells
    gain = gain_ref[...]
    head = gain.shape[1]
    for h in range(text_ref.shape[1] // head):
        part = text_ref[:, h * head : (h + 1) * head].astype(f32)
        mean = jnp.sum(part * part, -1, keepdims=True) * (1.0 / head)
        text_out_ref[:, h * head : (h + 1) * head] = (
            part * lax.rsqrt(mean + epsilon) * gain
        ).astype(bf16)

    even = lax.axis_index("seq") % 2 == 0
    up = jnp.where(even, far_ref[...], near_ref[...])
    down = jnp.where(even, near_ref[...], far_ref[...])
    extended = jnp.concatenate([up, own_ref[...], down], 1)
    total = extended.shape[1]
    origin = own_lanes - cells
    lane = lax.broadcasted_iota(jnp.int32, (channels, lanes), 1) % cells

    def shifted(down, right):
        start = origin + down * cells + right
        moved = pltpu.roll(extended, (-start) % total, 1)[:, :lanes]
        if right < 0:
            moved = jnp.where(lane == 0, 0.0, moved)
        if right > 0:
            moved = jnp.where(lane == cells - 1, 0.0, moved)
        return moved

    around = {(i, j): shifted(i, j) for i in (-1, 0, 1) for j in (-1, 0, 1)}

    taps = taps_ref[...].T
    same = lax.broadcasted_iota(jnp.int32, (channels, channels), 0) == lax.broadcasted_iota(
        jnp.int32, (channels, channels), 1
    )
    shift = jnp.sum(jnp.where(same, shift_ref[...], 0.0), 1, keepdims=True)

    def tap(r, s):
        first = (3 * r + s) * channels
        return taps[first : first + channels, :]

    blocks = {}
    for a in range(2):
        for c in range(2):
            patches, weights = [], []
            for i in (a - 1, a):
                for j in (c - 1, c):
                    merged = None
                    for r in range(3):
                        for s in range(3):
                            if (a + r - 1) // 2 == i and (c + s - 1) // 2 == j:
                                merged = tap(r, s) if merged is None else merged + tap(r, s)
                    patches.append(around[i, j])
                    weights.append(merged)
            stacked = jnp.concatenate(weights, 0).T
            product = jnp.dot(
                stacked, jnp.concatenate(patches, 0), precision=highest, preferred_element_type=f32
            )
            blocks[a, c] = product + shift + around[0, 0]

    embed, bias = centred_embedding(embed_ref[...].astype(f32), bias_ref[...])
    high, low = split(with_tail(embed, bias, jnp.zeros_like(bias)))
    pair = jnp.concatenate([high, low], 0)
    width = embed.shape[1]
    step = min(width, 512)

    def features(tokens):
        count = tokens.shape[1]
        one = jnp.ones((1, count), f32)
        values = with_tail(tokens.astype(f32), one, jnp.zeros_like(one)).astype(bf16)
        double = jnp.concatenate([values, values], 0)
        square = jnp.zeros((1, count), f32)
        for first in range(0, width, step):
            state = dot_rows(pair[:, first : first + step], double)
            square += jnp.sum(state * state, 0, keepdims=True)
        spread = lax.rsqrt(square * (1.0 / width) + epsilon)
        top, rest = split(with_tail(tokens.astype(f32) * spread, spread, one))
        fill = jnp.zeros((DEPTH - 3 * SLAB, count), bf16)
        return jnp.concatenate([top, rest, top, fill], 0)

    for a in range(2):
        for c in range(2):
            turned = features(blocks[a, c].astype(bf16)).T
            for r in range(rows + 2):
                first = (4 * r + 2 * a + c) * cells
                keys_ref[first : first + cells, :] = turned[r * cells : (r + 1) * cells, :]
    keys_t_ref[...] = keys_ref[...].T

    parity = lax.axis_index("cfg")
    tokens = jnp.zeros((channels, 2 * own_lanes), f32)
    cell = lax.broadcasted_iota(jnp.int32, (own_lanes, 2 * own_lanes), 0)
    place = lax.broadcasted_iota(jnp.int32, (own_lanes, 2 * own_lanes), 1)
    group = 128 // channels
    fine_lines = 2 * own_lanes // group
    line = lax.broadcasted_iota(jnp.int32, (fine_lines, own_lanes), 0)
    column = lax.broadcasted_iota(jnp.int32, (fine_lines, own_lanes), 1)
    belongs = jnp.where(line == 2 * column // group, 1.0, 0.0)
    lane128 = lax.broadcasted_iota(jnp.int32, (own_lanes, 128), 1) // channels
    cell128 = lax.broadcasted_iota(jnp.int32, (own_lanes, 128), 0)
    repeat = lane_repeat(channels)
    fine = jnp.zeros((own_lanes, 128), f32)
    for c in range(2):
        mine = jnp.where(parity == 0, blocks[0, c], blocks[1, c])
        mine = pltpu.roll(mine, lanes - cells, 1)[:, :own_lanes]
        fine += jnp.where(lane128 == (2 * cell128 + c) % group, exact(mine, repeat, (0, 0)), 0.0)
        chosen = jnp.where(place == 2 * cell + c, 1.0, 0.0).astype(bf16)
        tokens += jnp.dot(mine.astype(bf16), chosen, preferred_element_type=f32)
    fine_ref[...] = exact(belongs, fine, (1, 0))
    token_ref[...] = tokens.astype(bf16)
    query_ref[...] = features(tokens.astype(bf16)).T


def attend_kernel(
    rows,
    window,
    length_ref,
    keys_ref,
    keys_t_ref,
    query_ref,
    query_gain_ref,
    key_gain_ref,
    text_ref,
    text_values_ref,
    kept_any,
    other_any,
    out_ref,
    mix_ref,
    value_ref,
    gain_ref,
    kept_ref,
    other_ref,
    sems,
):
    step = pl.program_id(0)
    seq_index = lax.axis_index("seq")
    head = query_gain_ref.shape[1]
    half = kept_ref.shape[1]
    key_count = keys_ref.shape[0]
    text_count, span = text_ref.shape
    per_step = span // head
    inner = pl.num_programs(0) * span
    low_ok = seq_index > 0
    high_ok = seq_index < lax.axis_size("seq") - 1
    key_row = lax.broadcasted_iota(jnp.int32, (key_count, head), 0)
    allowed = (low_ok | (key_row >= window)) & (high_ok | (key_row < key_count - window))
    text_row = lax.broadcasted_iota(jnp.int32, (text_count, head), 0)
    text_allowed = text_row < length_ref[...]
    text_rows = slice(key_count, key_count + text_count)

    @pl.when(step == 0)
    def _():
        fetch([(kept_any, kept_ref), (other_any, other_ref)], sems)
        core = seq_index % 2
        mix_ref[...] = jnp.zeros_like(mix_ref)
        for side, part_ref in ((core, kept_ref), (1 - core, other_ref)):
            top, rest = split(part_ref[...])
            where = pl.ds(pl.multiple_of(side * half, 128), half)
            mix_ref[0:TERMS, where] = top
            mix_ref[SLAB : SLAB + TERMS, where] = top
            mix_ref[2 * SLAB : 2 * SLAB + TERMS, where] = rest
        for i in range(per_step):
            value_ref[i, 0:key_count, head : 2 * head] = jnp.where(allowed, 1.0, 0.0).astype(bf16)
            value_ref[i, text_rows, head : 2 * head] = jnp.where(text_allowed, 1.0, 0.0).astype(
                bf16
            )
        same = lax.broadcasted_iota(jnp.int32, (head, head), 0) == lax.broadcasted_iota(
            jnp.int32, (head, head), 1
        )
        column = jnp.sum(jnp.where(same, key_gain_ref[...], 0.0), 1, keepdims=True)
        gain_ref[...] = jnp.broadcast_to(column, gain_ref.shape)

    def columns(which):
        return pl.ds(pl.multiple_of(which * inner + step * span, 128), span)

    queries = jnp.dot(query_ref[...], mix_ref[:, columns(0)], preferred_element_type=f32)
    all_keys = dot_rows(mix_ref[:, columns(1)], keys_t_ref[...])
    values = jnp.dot(keys_ref[...], mix_ref[:, columns(2)], preferred_element_type=f32)
    factor = head ** (-0.5) * LOG2E
    tokens = queries.shape[0] // rows
    for i in range(per_step):
        mine = slice(i * head, (i + 1) * head)
        query = queries[:, mine]
        mean = jnp.sum(query * query, -1, keepdims=True) * (1.0 / head)
        query = (query * lax.rsqrt(mean + epsilon) * query_gain_ref[...]).astype(bf16)
        keys = all_keys[mine]
        mean = jnp.sum(keys * keys, 0, keepdims=True) * (1.0 / head)
        keys = (keys * lax.rsqrt(mean + epsilon) * gain_ref[:, 0:1]).astype(bf16)
        value_ref[i, 0:key_count, 0:head] = jnp.where(allowed, values[:, mine], 0.0).astype(bf16)
        value_ref[i, text_rows, 0:head] = jnp.where(
            text_allowed, text_values_ref[:, mine].astype(f32), 0.0
        ).astype(bf16)
        for r in range(rows):
            part = query[r * tokens : (r + 1) * tokens]
            near = slice(r * window, (r + 3) * window)
            scores = jnp.dot(part, keys[:, near], preferred_element_type=f32)
            text_scores = lax.dot_general(
                part, text_ref[:, mine], (((1,), (1,)), ((), ())), preferred_element_type=f32
            )
            mixed = jnp.dot(
                jnp.exp2(scores * factor).astype(bf16),
                value_ref[i, near, :],
                preferred_element_type=f32,
            ) + jnp.dot(
                jnp.exp2(text_scores * factor).astype(bf16),
                value_ref[i, text_rows, :],
                preferred_element_type=f32,
            )
            out_ref[r * tokens : (r + 1) * tokens, mine] = (mixed[:, :head] / mixed[:, head:]).astype(
                bf16
            )


def output_kernel(
    levels,
    last,
    attended_ref,
    token_ref,
    embed_ref,
    bias_ref,
    mod_ref,
    own_first_ref,
    own_second_ref,
    other_first_ref,
    other_second_ref,
    *rest,
):
    out_any, block_ref, sems = rest[-3:]
    count, piece, _ = own_first_ref.shape
    seq_index = lax.axis_index("seq")
    core = seq_index % 2
    low = len(levels) - 3
    seq_chips = lax.axis_size("seq") // 2
    attended = attended_ref[...]
    tokens = token_ref[...]
    lanes = 2 * piece
    sides = ((own_first_ref, other_first_ref), (own_second_ref, other_second_ref))
    group = 2
    copies = []
    for top, (own_ref, other_ref) in enumerate(sides):
        for start in range(0, count, group):
            blocks = []
            for index in range(start, start + group):
                blocks += [own_ref[index], other_ref[index]]
            product = lax.dot_general(
                attended,
                jnp.concatenate(blocks, 0),
                (((1,), (1,)), ((), ())),
                preferred_element_type=f32,
            )
            for i in range(group):
                index = start + i
                near = index >> low & 1
                first, second = (near, last) if top == 0 else (last, near)
                flip = second + (top << (levels[-1][1] - 1))
                for j in range(low):
                    flip = flip + ((index >> j & 1) << (levels[2 + j][1] - 1))
                chip = (lax.axis_index("cfg") ^ first) * seq_chips + (seq_index // 2 ^ flip)
                where = pl.ds(pl.multiple_of(chip * lanes, lanes), lanes)
                block = pltpu.roll(product[:, i * lanes : (i + 1) * lanes], core * piece, 1)
                state = dot_rows(tokens, embed_ref[:, where]) + bias_ref[:, where]
                slot = top * count + index
                block_ref[slot] = (state + mod_ref[2:3, where] * block).astype(bf16)
                copy = pltpu.make_async_copy(block_ref.at[slot], out_any.at[:, where], sems.at[slot])
                copy.start()
                copies.append(copy)
    for copy in copies:
        copy.wait()


def per_device(
    coarse_hidden,
    coarse_modulation,
    final_weight,
    coarse_latent,
    step_index,
    guide_index,
    guide_scales,
    upsample_weight,
    upsample_bias,
    embed_weight,
    embed_bias,
    fine_modulation,
    project_weight,
    query_gain,
    key_gain,
    text_keys,
    text_values,
    text_length,
    output_weight,
):
    rows = coarse_hidden.shape[1]
    cells = coarse_hidden.shape[2]
    width = coarse_hidden.shape[3]
    channels = final_weight.shape[1]
    head = query_gain.shape[0]
    inner = project_weight.shape[1] // 3
    cfg_count = lax.axis_size("cfg")
    seq_count = lax.axis_size("seq")
    seq_index = lax.axis_index("seq")
    seq_bits = seq_count.bit_length() - 1
    assert seq_count == 1 << seq_bits and cfg_count == 2 and rows >= 2 and seq_bits >= 3
    own = rows * cells
    fine_tokens = 2 * own
    key_count = (rows + 2) * 4 * cells
    text_count = text_keys.shape[0]
    bias_row = embed_bias.reshape(1, width)

    def swap(value, *stages):
        size = cfg_count * seq_count
        flip = 0
        for axis, bit in stages:
            flip |= seq_count if axis == "cfg" else 1 << bit
        return lax.ppermute(value, ("cfg", "seq"), [(i, i ^ flip) for i in range(size)])

    across = ("seq", 0)
    levels = [("cfg", 0)] + [("seq", bit) for bit in range(1, seq_bits)]

    half = 3 * inner // 2
    kept, sent = pl.pallas_call(
        functools.partial(partial_kernel, seq_count),
        out_shape=(jax.ShapeDtypeStruct((TERMS, half), f32),) * 2,
        in_specs=vmem(4),
        out_specs=tuple(vmem(2)),
        cost_estimate=cost(2e9, 1e6),
        name="partial_mix",
    )(embed_weight, bias_row, fine_modulation, project_weight)
    met = swap(sent, across)

    velocity = pl.pallas_call(
        velocity_kernel,
        out_shape=jax.ShapeDtypeStruct((channels, own), f32),
        in_specs=vmem(3),
        out_specs=vmem(1)[0],
        cost_estimate=cost(2e9, 1e6),
        name="velocity",
        compiler_params=pltpu.CompilerParams(vmem_limit_bytes=6 << 20),
    )(coarse_hidden.reshape(own, width), coarse_modulation[0], final_weight.T)
    partner = swap(velocity, ("cfg", 0))

    held = output_weight.T[None]

    def doubled(block, stage):
        return jnp.concatenate([block, swap(block, stage)], 0)

    first, second = levels[0], levels[1]
    total = kept + met
    rounded = total.astype(bf16)
    for stage in levels[2:]:
        held = doubled(held, stage)
    total = (
        total
        + swap(rounded, first).astype(f32)
        + swap(rounded, second).astype(f32)
        + swap(rounded, first, second).astype(f32)
    )

    lines = own * channels // 128
    latent = coarse_latent.reshape(rows, lines // rows, 128).transpose(1, 0, 2).reshape(lines, 128)
    guided, stepped = pl.pallas_call(
        functools.partial(guide_kernel, rows),
        out_shape=(
            jax.ShapeDtypeStruct((lines, 128), f32),
            jax.ShapeDtypeStruct((channels, own), f32),
        ),
        in_specs=vmem(4) + anywhere(2),
        out_specs=tuple(vmem(2)),
        scratch_shapes=[pltpu.VMEM((channels, own), f32)] * 2 + [pltpu.SemaphoreType.DMA((2,))],
        cost_estimate=cost(1e9, 1e5),
        name="guide",
        compiler_params=pltpu.CompilerParams(vmem_limit_bytes=2 << 20),
    )(
        step_index.reshape(1, 1),
        guide_index.reshape(1, 1),
        guide_scales.reshape(-1, 128),
        latent,
        velocity,
        partner,
    )

    near_rows = swap(stepped, across)
    ahead = [(i, i + 1) for i in range(1, seq_count - 1, 2)]
    behind = [(target, source) for source, target in ahead]
    far_rows = lax.ppermute(stepped, "seq", ahead + behind)

    fine, keys, keys_t, query, tokens, text_normed = pl.pallas_call(
        functools.partial(fine_kernel, cells),
        out_shape=(
            jax.ShapeDtypeStruct((2 * lines, 128), f32),
            jax.ShapeDtypeStruct((key_count, DEPTH), bf16),
            jax.ShapeDtypeStruct((DEPTH, key_count), bf16),
            jax.ShapeDtypeStruct((fine_tokens, DEPTH), bf16),
            jax.ShapeDtypeStruct((channels, fine_tokens), bf16),
            jax.ShapeDtypeStruct(text_keys.shape, bf16),
        ),
        in_specs=vmem(6) + anywhere(3),
        out_specs=tuple(vmem(6)),
        scratch_shapes=[pltpu.VMEM((channels, own), f32)] * 3 + [pltpu.SemaphoreType.DMA((3,))],
        cost_estimate=cost(4e9, 4e6),
        name="fine_features",
        compiler_params=pltpu.CompilerParams(vmem_limit_bytes=20 << 20),
    )(
        upsample_weight.T,
        upsample_bias.reshape(1, channels),
        embed_weight,
        bias_row,
        text_keys,
        key_gain.reshape(1, head),
        near_rows,
        stepped,
        far_rows,
    )

    for stage in levels[2:]:
        moved = swap(total.astype(bf16), stage)
        total = total + moved.astype(f32)
    others = swap(total, across)

    middle = held.shape[0] // 2
    own_first, own_second = held[:middle], held[middle:]
    own_first = doubled(own_first, first)
    own_second = doubled(own_second, second)
    far_first = swap(own_first, second)
    far_second = swap(own_second, first)
    near_pieces = (own_first, own_second, swap(own_first, across), swap(own_second, across))
    far_pieces = (far_first, far_second, swap(far_first, across), swap(far_second, across))

    whole = pl.BlockSpec(memory_space=pltpu.VMEM)
    free = pl.BlockSpec(memory_space=pl.ANY)
    span = 2 * head
    per_step = pl.BlockSpec((text_count, span), lambda h: (0, h))
    attended = pl.pallas_call(
        functools.partial(attend_kernel, rows, 4 * cells),
        grid=(inner // span,),
        out_shape=jax.ShapeDtypeStruct((fine_tokens, inner), bf16),
        in_specs=[whole] * 6 + [per_step, per_step, free, free],
        out_specs=pl.BlockSpec((fine_tokens, span), lambda h: (0, h)),
        scratch_shapes=[
            pltpu.VMEM((DEPTH, 3 * inner), bf16),
            pltpu.VMEM((2, key_count + text_count, 2 * head), bf16),
            pltpu.VMEM((head, 128), f32),
            pltpu.VMEM((TERMS, half), f32),
            pltpu.VMEM((TERMS, half), f32),
            pltpu.SemaphoreType.DMA((2,)),
        ],
        cost_estimate=cost(8e9, 4e6),
        name="attend",
        compiler_params=pltpu.CompilerParams(vmem_limit_bytes=24 << 20),
    )(
        text_length.reshape(1, 1),
        keys,
        keys_t,
        query,
        query_gain.reshape(1, head),
        key_gain.reshape(1, head),
        text_normed,
        text_values,
        total,
        others,
    )

    piece = output_weight.shape[1]
    count = own_first.shape[0]
    if 2 * piece == 128:

        def output(last, pieces, *before):
            return pl.pallas_call(
                functools.partial(output_kernel, tuple(levels), last),
                out_shape=jax.ShapeDtypeStruct((fine_tokens, width), bf16),
                in_specs=[whole] * 9 + [free] * len(before),
                out_specs=free,
                input_output_aliases={9: 0} if before else {},
                scratch_shapes=[
                    pltpu.VMEM((2 * count, fine_tokens, 128), bf16),
                    pltpu.SemaphoreType.DMA((2 * count,)),
                ],
                cost_estimate=cost(1e9, 3e6),
                compiler_params=pltpu.CompilerParams(vmem_limit_bytes=16 << 20),
            )(attended, tokens, embed_weight, bias_row, fine_modulation, *pieces, *before)

        near = output(0, near_pieces)
        hidden = output(1, far_pieces, near)
    else:
        low = len(levels) - 3
        chip = jnp.arange(4 * count, dtype=jnp.int32)
        seq_chips = seq_count // 2
        apart = chip // seq_chips ^ lax.axis_index("cfg")
        flip = chip % seq_chips ^ seq_index // 2
        side = flip & 1
        top = flip >> (levels[-1][1] - 1) & 1
        position = top * count + (jnp.where(top == 0, apart, side) << low)
        position = position + jnp.where(top == 0, side, apart) * (2 * count)
        for j in range(low):
            position = position + ((flip >> (levels[2 + j][1] - 1) & 1) << j)
        mine = jnp.take(jnp.concatenate(near_pieces[:2] + far_pieces[:2], 0), position, axis=0)
        theirs = jnp.take(jnp.concatenate(near_pieces[2:] + far_pieces[2:], 0), position, axis=0)
        even = seq_index % 2 == 0
        both = jnp.stack([jnp.where(even, mine, theirs), jnp.where(even, theirs, mine)], 1)
        product = lax.dot_general(
            attended,
            both.reshape(width, inner),
            (((1,), (1,)), ((), ())),
            preferred_element_type=f32,
        )
        state = dot_rows(tokens, embed_weight) + bias_row
        hidden = (state + fine_modulation[2:3] * product).astype(bf16)

    guided = guided.reshape(lines // rows, rows, 128).transpose(1, 0, 2)
    return (
        guided.reshape(rows, cells * channels),
        fine.reshape(rows, 1, 2 * cells * channels),
        hidden.reshape(rows, 1, 2 * cells, width),
    )


def solution(mesh):
    placed = (
        P("cfg", "seq", None, None),
        P("cfg", None, None),
        P(),
        P("seq", None),
        P(),
        P(),
        P(),
        P(),
        P(),
        P(),
        P(),
        P(),
        P(("cfg", "seq"), None),
        P(),
        P(),
        P(),
        P(),
        P(),
        P(None, ("cfg", "seq")),
    )
    return jax.shard_map(
        per_device,
        mesh=mesh,
        in_specs=placed,
        out_specs=(P("seq", None), P("seq", "cfg", None), P("seq", "cfg", None, None)),
        check_vma=False,
    )
```

```python
import functools

import jax
import jax.numpy as jnp
from jax import lax
from jax.experimental import pallas as pl
from jax.experimental.pallas import tpu as pltpu
from jax.sharding import PartitionSpec as P

STEPS = 50

epsilon = 1e-06
flow_shift = 5.0
highest = lax.Precision.HIGHEST
f32 = jnp.float32
bf16 = jnp.bfloat16
LOG2E = 1.4426950408889634
TERMS = 40
SLAB = 48
DEPTH = 256


def vmem(count):
    return [pl.BlockSpec(memory_space=pltpu.VMEM) for _ in range(count)]


def cost(flops, moved):
    return pl.CostEstimate(flops=int(flops), bytes_accessed=int(moved), transcendentals=0)


def dot_rows(left, right):
    return lax.dot_general(left, right, (((0,), (0,)), ((), ())), preferred_element_type=f32)


def anywhere(count):
    return [pl.BlockSpec(memory_space=pl.ANY) for _ in range(count)]


def fetch(pairs, sems):
    copies = [pltpu.make_async_copy(src, dst, sems.at[i]) for i, (src, dst) in enumerate(pairs)]
    for copy in copies:
        copy.start()
    for copy in copies:
        copy.wait()


def exact(left, right, contract):
    return lax.dot_general(
        left, right, ((contract[:1], contract[1:]), ((), ())), precision=highest,
        preferred_element_type=f32,
    )


def lane_repeat(channels):
    lane = lax.broadcasted_iota(jnp.int32, (channels, 128), 1)
    row = lax.broadcasted_iota(jnp.int32, (channels, 128), 0)
    return jnp.where(lane % channels == row, 1.0, 0.0)


def split(values):
    high = values.astype(bf16)
    return high, (values - high.astype(f32)).astype(bf16)


def centred_embedding(embed, bias):
    width = embed.shape[1]
    embed = embed - jnp.sum(embed, -1, keepdims=True) * (1.0 / width)
    bias = bias - jnp.sum(bias, -1, keepdims=True) * (1.0 / width)
    return embed, bias


def with_tail(body, first, second):
    row = lax.broadcasted_iota(jnp.int32, (16, body.shape[1]), 0)
    tail = jnp.where(row == 0, first, jnp.where(row == 1, second, 0.0))
    return jnp.concatenate([body, tail], 0)


def partial_kernel(seq_count, embed_ref, bias_ref, mod_ref, weight_ref, keep_ref, send_ref):
    seq_index = lax.axis_index("seq")
    core = seq_index % 2
    depth = weight_ref.shape[0]
    half = keep_ref.shape[1]
    embed = embed_ref[...].astype(f32)
    width = embed.shape[1]
    embed_mean = jnp.sum(embed, -1, keepdims=True) * (1.0 / width)
    bias_mean = jnp.sum(bias_ref[...], -1, keepdims=True) * (1.0 / width)
    start = (lax.axis_index("cfg") * seq_count + seq_index) * depth
    base = pl.multiple_of(start // 128 * 128, 128)
    offset = start - base
    window = pl.ds(base, 128)
    scale = 1.0 + mod_ref[1:2, window]
    rows = with_tail(
        (embed_ref[:, window].astype(f32) - embed_mean) * scale,
        (bias_ref[:, window] - bias_mean) * scale,
        mod_ref[0:1, window],
    )
    rows = pltpu.roll(rows, (128 - offset) % 128, 1)[:, :depth]
    high, low = split(rows)
    left = jnp.concatenate([high, low], 0)

    def part(which):
        columns = pl.ds(pl.multiple_of(which * half, 128), half)
        product = jnp.dot(left, weight_ref[:, columns], preferred_element_type=f32)
        return product[:TERMS] + product[SLAB : SLAB + TERMS]

    send_ref[...] = part(1 - core)
    keep_ref[...] = part(core)


def velocity_kernel(
    hidden_ref, mod_ref, weight_ref, shift_ref, key_gain_ref, query_gain_ref, out_ref, small_ref
):
    small_ref[...] = jnp.zeros_like(small_ref)
    small_ref[0:1, 0 : shift_ref.shape[1]] = shift_ref[...]
    small_ref[1:2, :] = key_gain_ref[...]
    small_ref[2:3, :] = query_gain_ref[...]
    values = hidden_ref[...].astype(f32)
    width = values.shape[1]
    centred = values - jnp.sum(values, -1, keepdims=True) * (1.0 / width)
    variance = jnp.sum(centred * centred, -1, keepdims=True) * (1.0 / width)
    normed = centred * lax.rsqrt(variance + epsilon)
    modulated = (normed * (1.0 + mod_ref[1:2, :]) + mod_ref[0:1, :]).astype(bf16)
    out_ref[...] = lax.dot_general(
        weight_ref[...], modulated, (((1,), (1,)), ((), ())), preferred_element_type=f32
    )


def guide_kernel(
    rows,
    table_ref,
    latent_ref,
    step_any,
    slot_any,
    own_any,
    other_any,
    guided_ref,
    next_ref,
    step_ref,
    slot_ref,
    own_ref,
    other_ref,
    sems,
):
    fetch(
        [(step_any, step_ref), (slot_any, slot_ref), (own_any, own_ref), (other_any, other_ref)], sems
    )
    branch = lax.axis_index("cfg")
    own = own_ref[...]
    other = other_ref[...]
    channels, count = own.shape
    group = 128 // channels
    cells = count // rows
    line = lax.broadcasted_iota(jnp.int32, (count // group, count), 0)
    column = lax.broadcasted_iota(jnp.int32, (count // group, count), 1)
    belongs = jnp.where(line == column % cells // group * rows + column // cells, 1.0, 0.0)
    lane = lax.broadcasted_iota(jnp.int32, (count, 128), 1)
    cell = lax.broadcasted_iota(jnp.int32, (count, 128), 0)
    slot = lane // channels == cell % group
    repeat = lane_repeat(channels)
    spread = jnp.where(slot, exact(belongs, latent_ref[...], (0, 0)), 0.0)
    latent = exact(repeat, spread, (1, 1))
    first = branch == 0
    conditional = jnp.where(first, own, other)
    unconditional = jnp.where(first, other, own)
    table = table_ref[...]
    slots = lax.broadcasted_iota(jnp.int32, table.shape, 0) * table.shape[
        1
    ] + lax.broadcasted_iota(jnp.int32, table.shape, 1)
    picked = jnp.where(slots == slot_ref[0], table, 0.0)
    guidance = jnp.sum(jnp.sum(picked, 0, keepdims=True), 1, keepdims=True)
    guided = unconditional + guidance * (conditional - unconditional)

    def sigma(step):
        fraction = 1.0 - jnp.full((1, 1), step, jnp.int32).astype(f32) / STEPS
        return flow_shift * fraction / (1.0 + (flow_shift - 1.0) * fraction)

    change = sigma(step_ref[0] + 1) - sigma(step_ref[0])
    next_ref[...] = latent + change * guided
    guided_ref[...] = exact(belongs, jnp.where(slot, exact(guided, repeat, (0, 0)), 0.0), (1, 0))


def fine_kernel(
    cells,
    taps_ref,
    small_ref,
    embed_ref,
    bias_ref,
    text_ref,
    near_any,
    own_any,
    far_any,
    fine_ref,
    keys_ref,
    keys_t_ref,
    query_ref,
    token_ref,
    text_out_ref,
    near_ref,
    own_ref,
    far_ref,
    sems,
):
    fetch([(near_any, near_ref), (own_any, own_ref), (far_any, far_ref)], sems)
    channels, own_lanes = own_ref.shape
    rows = own_lanes // cells
    lanes = (rows + 2) * cells
    gain = small_ref[1:2, :]
    head = gain.shape[1]
    for h in range(text_ref.shape[1] // head):
        part = text_ref[:, h * head : (h + 1) * head].astype(f32)
        mean = jnp.sum(part * part, -1, keepdims=True) * (1.0 / head)
        text_out_ref[:, h * head : (h + 1) * head] = (
            part * lax.rsqrt(mean + epsilon) * gain
        ).astype(bf16)

    even = lax.axis_index("seq") % 2 == 0
    up = jnp.where(even, far_ref[...], near_ref[...])
    down = jnp.where(even, near_ref[...], far_ref[...])
    extended = jnp.concatenate([up, own_ref[...], down], 1)
    total = extended.shape[1]
    origin = own_lanes - cells
    lane = lax.broadcasted_iota(jnp.int32, (channels, lanes), 1) % cells

    def shifted(down, right):
        start = origin + down * cells + right
        moved = pltpu.roll(extended, (-start) % total, 1)[:, :lanes]
        if right < 0:
            moved = jnp.where(lane == 0, 0.0, moved)
        if right > 0:
            moved = jnp.where(lane == cells - 1, 0.0, moved)
        return moved

    around = {(i, j): shifted(i, j) for i in (-1, 0, 1) for j in (-1, 0, 1)}

    taps = taps_ref[...].T
    same = lax.broadcasted_iota(jnp.int32, (channels, channels), 0) == lax.broadcasted_iota(
        jnp.int32, (channels, channels), 1
    )
    shift = jnp.sum(jnp.where(same, small_ref[0:1, :channels], 0.0), 1, keepdims=True)

    def tap(r, s):
        first = (3 * r + s) * channels
        return taps[first : first + channels, :]

    blocks = {}
    for a in range(2):
        for c in range(2):
            patches, weights = [], []
            for i in (a - 1, a):
                for j in (c - 1, c):
                    merged = None
                    for r in range(3):
                        for s in range(3):
                            if (a + r - 1) // 2 == i and (c + s - 1) // 2 == j:
                                merged = tap(r, s) if merged is None else merged + tap(r, s)
                    patches.append(around[i, j])
                    weights.append(merged)
            stacked = jnp.concatenate(weights, 0).T
            product = jnp.dot(
                stacked, jnp.concatenate(patches, 0), precision=highest, preferred_element_type=f32
            )
            blocks[a, c] = product + shift + around[0, 0]

    embed, bias = centred_embedding(embed_ref[...].astype(f32), bias_ref[...])
    high, low = split(with_tail(embed, bias, jnp.zeros_like(bias)))
    pair = jnp.concatenate([high, low], 0)
    width = embed.shape[1]
    step = min(width, 512)

    def features(tokens):
        count = tokens.shape[1]
        one = jnp.ones((1, count), f32)
        values = with_tail(tokens.astype(f32), one, jnp.zeros_like(one)).astype(bf16)
        double = jnp.concatenate([values, values], 0)
        square = jnp.zeros((1, count), f32)
        for first in range(0, width, step):
            state = dot_rows(pair[:, first : first + step], double)
            square += jnp.sum(state * state, 0, keepdims=True)
        spread = lax.rsqrt(square * (1.0 / width) + epsilon)
        top, rest = split(with_tail(tokens.astype(f32) * spread, spread, one))
        fill = jnp.zeros((DEPTH - 3 * SLAB, count), bf16)
        return jnp.concatenate([top, rest, top, fill], 0)

    for a in range(2):
        for c in range(2):
            turned = features(blocks[a, c].astype(bf16)).T
            for r in range(rows + 2):
                first = (4 * r + 2 * a + c) * cells
                keys_ref[first : first + cells, :] = turned[r * cells : (r + 1) * cells, :]
    keys_t_ref[...] = keys_ref[...].T

    parity = lax.axis_index("cfg")
    tokens = jnp.zeros((channels, 2 * own_lanes), f32)
    cell = lax.broadcasted_iota(jnp.int32, (own_lanes, 2 * own_lanes), 0)
    place = lax.broadcasted_iota(jnp.int32, (own_lanes, 2 * own_lanes), 1)
    group = 128 // channels
    fine_lines = 2 * own_lanes // group
    line = lax.broadcasted_iota(jnp.int32, (fine_lines, own_lanes), 0)
    column = lax.broadcasted_iota(jnp.int32, (fine_lines, own_lanes), 1)
    belongs = jnp.where(line == 2 * column // group, 1.0, 0.0)
    lane128 = lax.broadcasted_iota(jnp.int32, (own_lanes, 128), 1) // channels
    cell128 = lax.broadcasted_iota(jnp.int32, (own_lanes, 128), 0)
    repeat = lane_repeat(channels)
    fine = jnp.zeros((own_lanes, 128), f32)
    for c in range(2):
        mine = jnp.where(parity == 0, blocks[0, c], blocks[1, c])
        mine = pltpu.roll(mine, lanes - cells, 1)[:, :own_lanes]
        fine += jnp.where(lane128 == (2 * cell128 + c) % group, exact(mine, repeat, (0, 0)), 0.0)
        chosen = jnp.where(place == 2 * cell + c, 1.0, 0.0).astype(bf16)
        tokens += jnp.dot(mine.astype(bf16), chosen, preferred_element_type=f32)
    fine_ref[...] = exact(belongs, fine, (1, 0))
    token_ref[...] = tokens.astype(bf16)
    query_ref[...] = features(tokens.astype(bf16)).T


def attend_kernel(
    rows,
    window,
    keys_ref,
    keys_t_ref,
    query_ref,
    small_ref,
    text_ref,
    text_values_ref,
    length_any,
    kept_any,
    other_any,
    out_ref,
    mix_ref,
    value_ref,
    gain_ref,
    length_ref,
    kept_ref,
    other_ref,
    sems,
):
    step = pl.program_id(0)
    seq_index = lax.axis_index("seq")
    head = small_ref.shape[1]
    half = kept_ref.shape[1]
    key_count = keys_ref.shape[0]
    text_count, span = text_ref.shape
    per_step = span // head
    inner = pl.num_programs(0) * span
    low_ok = seq_index > 0
    high_ok = seq_index < lax.axis_size("seq") - 1
    key_row = lax.broadcasted_iota(jnp.int32, (key_count, head), 0)
    allowed = (low_ok | (key_row >= window)) & (high_ok | (key_row < key_count - window))
    text_row = lax.broadcasted_iota(jnp.int32, (text_count, head), 0)
    text_rows = slice(key_count, key_count + text_count)

    @pl.when(step == 0)
    def _():
        fetch([(length_any, length_ref), (kept_any, kept_ref), (other_any, other_ref)], sems)
        text_allowed = text_row < length_ref[0]
        core = seq_index % 2
        mix_ref[...] = jnp.zeros_like(mix_ref)
        for side, part_ref in ((core, kept_ref), (1 - core, other_ref)):
            top, rest = split(part_ref[...])
            where = pl.ds(pl.multiple_of(side * half, 128), half)
            mix_ref[0:TERMS, where] = top
            mix_ref[SLAB : SLAB + TERMS, where] = top
            mix_ref[2 * SLAB : 2 * SLAB + TERMS, where] = rest
        for i in range(per_step):
            value_ref[i, 0:key_count, head : 2 * head] = jnp.where(allowed, 1.0, 0.0).astype(bf16)
            value_ref[i, text_rows, head : 2 * head] = jnp.where(text_allowed, 1.0, 0.0).astype(
                bf16
            )
        same = lax.broadcasted_iota(jnp.int32, (head, head), 0) == lax.broadcasted_iota(
            jnp.int32, (head, head), 1
        )
        column = jnp.sum(jnp.where(same, small_ref[1:2, :], 0.0), 1, keepdims=True)
        gain_ref[...] = jnp.broadcast_to(column, gain_ref.shape)

    text_allowed = text_row < length_ref[0]

    def columns(which):
        return pl.ds(pl.multiple_of(which * inner + step * span, 128), span)

    queries = jnp.dot(query_ref[...], mix_ref[:, columns(0)], preferred_element_type=f32)
    all_keys = dot_rows(mix_ref[:, columns(1)], keys_t_ref[...])
    values = jnp.dot(keys_ref[...], mix_ref[:, columns(2)], preferred_element_type=f32)
    factor = head ** (-0.5) * LOG2E
    tokens = queries.shape[0] // rows
    for i in range(per_step):
        mine = slice(i * head, (i + 1) * head)
        query = queries[:, mine]
        mean = jnp.sum(query * query, -1, keepdims=True) * (1.0 / head)
        query = (query * lax.rsqrt(mean + epsilon) * small_ref[2:3, :]).astype(bf16)
        keys = all_keys[mine]
        mean = jnp.sum(keys * keys, 0, keepdims=True) * (1.0 / head)
        keys = (keys * lax.rsqrt(mean + epsilon) * gain_ref[:, 0:1]).astype(bf16)
        value_ref[i, 0:key_count, 0:head] = jnp.where(allowed, values[:, mine], 0.0).astype(bf16)
        value_ref[i, text_rows, 0:head] = jnp.where(
            text_allowed, text_values_ref[:, mine].astype(f32), 0.0
        ).astype(bf16)
        for r in range(rows):
            part = query[r * tokens : (r + 1) * tokens]
            near = slice(r * window, (r + 3) * window)
            scores = jnp.dot(part, keys[:, near], preferred_element_type=f32)
            text_scores = lax.dot_general(
                part, text_ref[:, mine], (((1,), (1,)), ((), ())), preferred_element_type=f32
            )
            mixed = jnp.dot(
                jnp.exp2(scores * factor).astype(bf16),
                value_ref[i, near, :],
                preferred_element_type=f32,
            ) + jnp.dot(
                jnp.exp2(text_scores * factor).astype(bf16),
                value_ref[i, text_rows, :],
                preferred_element_type=f32,
            )
            out_ref[r * tokens : (r + 1) * tokens, mine] = (mixed[:, :head] / mixed[:, head:]).astype(
                bf16
            )


def output_kernel(
    levels,
    last,
    attended_ref,
    token_ref,
    embed_ref,
    bias_ref,
    mod_ref,
    own_first_ref,
    own_second_ref,
    other_first_ref,
    other_second_ref,
    *rest,
):
    out_any, block_ref, sems = rest[-3:]
    count, piece, _ = own_first_ref.shape
    seq_index = lax.axis_index("seq")
    core = seq_index % 2
    low = len(levels) - 3
    seq_chips = lax.axis_size("seq") // 2
    attended = attended_ref[...]
    tokens = token_ref[...]
    lanes = 2 * piece
    sides = ((own_first_ref, other_first_ref), (own_second_ref, other_second_ref))
    group = 2
    copies = []
    for top, (own_ref, other_ref) in enumerate(sides):
        for start in range(0, count, group):
            blocks = []
            for index in range(start, start + group):
                blocks += [own_ref[index], other_ref[index]]
            product = lax.dot_general(
                attended,
                jnp.concatenate(blocks, 0),
                (((1,), (1,)), ((), ())),
                preferred_element_type=f32,
            )
            for i in range(group):
                index = start + i
                near = index >> low & 1
                first, second = (near, last) if top == 0 else (last, near)
                flip = second + (top << (levels[-1][1] - 1))
                for j in range(low):
                    flip = flip + ((index >> j & 1) << (levels[2 + j][1] - 1))
                chip = (lax.axis_index("cfg") ^ first) * seq_chips + (seq_index // 2 ^ flip)
                where = pl.ds(pl.multiple_of(chip * lanes, lanes), lanes)
                block = pltpu.roll(product[:, i * lanes : (i + 1) * lanes], core * piece, 1)
                state = dot_rows(tokens, embed_ref[:, where]) + bias_ref[:, where]
                slot = top * count + index
                block_ref[slot] = (state + mod_ref[2:3, where] * block).astype(bf16)
                copy = pltpu.make_async_copy(block_ref.at[slot], out_any.at[:, where], sems.at[slot])
                copy.start()
                copies.append(copy)
    for copy in copies:
        copy.wait()


def per_device(
    coarse_hidden,
    coarse_modulation,
    final_weight,
    coarse_latent,
    step_index,
    guide_index,
    guide_scales,
    upsample_weight,
    upsample_bias,
    embed_weight,
    embed_bias,
    fine_modulation,
    project_weight,
    query_gain,
    key_gain,
    text_keys,
    text_values,
    text_length,
    output_weight,
):
    rows = coarse_hidden.shape[1]
    cells = coarse_hidden.shape[2]
    width = coarse_hidden.shape[3]
    channels = final_weight.shape[1]
    head = query_gain.shape[0]
    inner = project_weight.shape[1] // 3
    cfg_count = lax.axis_size("cfg")
    seq_count = lax.axis_size("seq")
    seq_index = lax.axis_index("seq")
    seq_bits = seq_count.bit_length() - 1
    assert seq_count == 1 << seq_bits and cfg_count == 2 and rows >= 2 and seq_bits >= 3
    own = rows * cells
    fine_tokens = 2 * own
    key_count = (rows + 2) * 4 * cells
    text_count = text_keys.shape[0]
    bias_row = embed_bias.reshape(1, width)

    def swap(value, *stages):
        size = cfg_count * seq_count
        flip = 0
        for axis, bit in stages:
            flip |= seq_count if axis == "cfg" else 1 << bit
        return lax.ppermute(value, ("cfg", "seq"), [(i, i ^ flip) for i in range(size)])

    across = ("seq", 0)
    levels = [("cfg", 0)] + [("seq", bit) for bit in range(1, seq_bits)]

    half = 3 * inner // 2
    kept, sent = pl.pallas_call(
        functools.partial(partial_kernel, seq_count),
        out_shape=(jax.ShapeDtypeStruct((TERMS, half), f32),) * 2,
        in_specs=vmem(4),
        out_specs=tuple(vmem(2)),
        cost_estimate=cost(2e9, 1e6),
        name="partial_mix",
    )(embed_weight, bias_row, fine_modulation, project_weight)
    met = swap(sent, across)

    velocity, small = pl.pallas_call(
        velocity_kernel,
        out_shape=(
            jax.ShapeDtypeStruct((channels, own), f32),
            jax.ShapeDtypeStruct((8, head), f32),
        ),
        in_specs=vmem(6),
        out_specs=tuple(vmem(2)),
        cost_estimate=cost(2e9, 1e6),
        name="velocity",
        compiler_params=pltpu.CompilerParams(vmem_limit_bytes=6 << 20),
    )(
        coarse_hidden.reshape(own, width),
        coarse_modulation[0],
        final_weight.T,
        upsample_bias.reshape(1, channels),
        key_gain.reshape(1, head),
        query_gain.reshape(1, head),
    )
    partner = swap(velocity, ("cfg", 0))

    held = output_weight.T[None]

    def doubled(block, stage):
        return jnp.concatenate([block, swap(block, stage)], 0)

    first, second = levels[0], levels[1]
    total = kept + met
    rounded = total.astype(bf16)
    for stage in levels[2:]:
        held = doubled(held, stage)
    total = (
        total
        + swap(rounded, first).astype(f32)
        + swap(rounded, second).astype(f32)
        + swap(rounded, first, second).astype(f32)
    )

    lines = own * channels // 128
    latent = coarse_latent.reshape(rows, lines // rows, 128).transpose(1, 0, 2).reshape(lines, 128)
    guided, stepped = pl.pallas_call(
        functools.partial(guide_kernel, rows),
        out_shape=(
            jax.ShapeDtypeStruct((lines, 128), f32),
            jax.ShapeDtypeStruct((channels, own), f32),
        ),
        in_specs=vmem(2) + anywhere(4),
        out_specs=tuple(vmem(2)),
        scratch_shapes=[pltpu.SMEM((1,), jnp.int32)] * 2
        + [pltpu.VMEM((channels, own), f32)] * 2
        + [pltpu.SemaphoreType.DMA((4,))],
        cost_estimate=cost(1e9, 1e5),
        name="guide",
        compiler_params=pltpu.CompilerParams(vmem_limit_bytes=2 << 20),
    )(
        guide_scales.reshape(-1, 128),
        latent,
        step_index,
        guide_index,
        velocity,
        partner,
    )

    near_rows = swap(stepped, across)
    ahead = [(i, i + 1) for i in range(1, seq_count - 1, 2)]
    behind = [(target, source) for source, target in ahead]
    far_rows = lax.ppermute(stepped, "seq", ahead + behind)

    fine, keys, keys_t, query, tokens, text_normed = pl.pallas_call(
        functools.partial(fine_kernel, cells),
        out_shape=(
            jax.ShapeDtypeStruct((2 * lines, 128), f32),
            jax.ShapeDtypeStruct((key_count, DEPTH), bf16),
            jax.ShapeDtypeStruct((DEPTH, key_count), bf16),
            jax.ShapeDtypeStruct((fine_tokens, DEPTH), bf16),
            jax.ShapeDtypeStruct((channels, fine_tokens), bf16),
            jax.ShapeDtypeStruct(text_keys.shape, bf16),
        ),
        in_specs=vmem(5) + anywhere(3),
        out_specs=tuple(vmem(6)),
        scratch_shapes=[pltpu.VMEM((channels, own), f32)] * 3 + [pltpu.SemaphoreType.DMA((3,))],
        cost_estimate=cost(4e9, 4e6),
        name="fine_features",
        compiler_params=pltpu.CompilerParams(vmem_limit_bytes=20 << 20),
    )(
        upsample_weight.T,
        small,
        embed_weight,
        bias_row,
        text_keys,
        near_rows,
        stepped,
        far_rows,
    )

    for stage in levels[2:]:
        moved = swap(total.astype(bf16), stage)
        total = total + moved.astype(f32)
    others = swap(total, across)

    middle = held.shape[0] // 2
    own_first, own_second = held[:middle], held[middle:]
    own_first = doubled(own_first, first)
    own_second = doubled(own_second, second)
    far_first = swap(own_first, second)
    far_second = swap(own_second, first)
    near_pieces = (own_first, own_second, swap(own_first, across), swap(own_second, across))
    far_pieces = (far_first, far_second, swap(far_first, across), swap(far_second, across))

    whole = pl.BlockSpec(memory_space=pltpu.VMEM)
    free = pl.BlockSpec(memory_space=pl.ANY)
    span = 2 * head
    per_step = pl.BlockSpec((text_count, span), lambda h: (0, h))
    attended = pl.pallas_call(
        functools.partial(attend_kernel, rows, 4 * cells),
        grid=(inner // span,),
        out_shape=jax.ShapeDtypeStruct((fine_tokens, inner), bf16),
        in_specs=[whole] * 4 + [per_step, per_step, free, free, free],
        out_specs=pl.BlockSpec((fine_tokens, span), lambda h: (0, h)),
        scratch_shapes=[
            pltpu.VMEM((DEPTH, 3 * inner), bf16),
            pltpu.VMEM((2, key_count + text_count, 2 * head), bf16),
            pltpu.VMEM((head, 128), f32),
            pltpu.SMEM((1,), jnp.int32),
            pltpu.VMEM((TERMS, half), f32),
            pltpu.VMEM((TERMS, half), f32),
            pltpu.SemaphoreType.DMA((3,)),
        ],
        cost_estimate=cost(8e9, 4e6),
        name="attend",
        compiler_params=pltpu.CompilerParams(vmem_limit_bytes=24 << 20),
    )(
        keys,
        keys_t,
        query,
        small,
        text_normed,
        text_values,
        text_length,
        total,
        others,
    )

    piece = output_weight.shape[1]
    count = own_first.shape[0]
    if 2 * piece == 128:

        def output(last, pieces, *before):
            return pl.pallas_call(
                functools.partial(output_kernel, tuple(levels), last),
                out_shape=jax.ShapeDtypeStruct((fine_tokens, width), bf16),
                in_specs=[whole] * 9 + [free] * len(before),
                out_specs=free,
                input_output_aliases={9: 0} if before else {},
                scratch_shapes=[
                    pltpu.VMEM((2 * count, fine_tokens, 128), bf16),
                    pltpu.SemaphoreType.DMA((2 * count,)),
                ],
                cost_estimate=cost(1e9, 3e6),
                compiler_params=pltpu.CompilerParams(vmem_limit_bytes=16 << 20),
            )(attended, tokens, embed_weight, bias_row, fine_modulation, *pieces, *before)

        near = output(0, near_pieces)
        hidden = output(1, far_pieces, near)
    else:
        low = len(levels) - 3
        chip = jnp.arange(4 * count, dtype=jnp.int32)
        seq_chips = seq_count // 2
        apart = chip // seq_chips ^ lax.axis_index("cfg")
        flip = chip % seq_chips ^ seq_index // 2
        side = flip & 1
        top = flip >> (levels[-1][1] - 1) & 1
        position = top * count + (jnp.where(top == 0, apart, side) << low)
        position = position + jnp.where(top == 0, side, apart) * (2 * count)
        for j in range(low):
            position = position + ((flip >> (levels[2 + j][1] - 1) & 1) << j)
        mine = jnp.take(jnp.concatenate(near_pieces[:2] + far_pieces[:2], 0), position, axis=0)
        theirs = jnp.take(jnp.concatenate(near_pieces[2:] + far_pieces[2:], 0), position, axis=0)
        even = seq_index % 2 == 0
        both = jnp.stack([jnp.where(even, mine, theirs), jnp.where(even, theirs, mine)], 1)
        product = lax.dot_general(
            attended,
            both.reshape(width, inner),
            (((1,), (1,)), ((), ())),
            preferred_element_type=f32,
        )
        state = dot_rows(tokens, embed_weight) + bias_row
        hidden = (state + fine_modulation[2:3] * product).astype(bf16)

    guided = guided.reshape(lines // rows, rows, 128).transpose(1, 0, 2)
    return (
        guided.reshape(rows, cells * channels),
        fine.reshape(rows, 1, 2 * cells * channels),
        hidden.reshape(rows, 1, 2 * cells, width),
    )


def solution(mesh):
    placed = (
        P("cfg", "seq", None, None),
        P("cfg", None, None),
        P(),
        P("seq", None),
        P(),
        P(),
        P(),
        P(),
        P(),
        P(),
        P(),
        P(),
        P(("cfg", "seq"), None),
        P(),
        P(),
        P(),
        P(),
        P(),
        P(None, ("cfg", "seq")),
    )
    return jax.shard_map(
        per_device,
        mesh=mesh,
        in_specs=placed,
        out_specs=(P("seq", None), P("seq", "cfg", None), P("seq", "cfg", None, None)),
        check_vma=False,
    )
```

```python
import functools

import jax
import jax.numpy as jnp
from jax import lax
from jax.experimental import pallas as pl
from jax.experimental.pallas import tpu as pltpu
from jax.sharding import PartitionSpec as P

STEPS = 50

epsilon = 1e-06
flow_shift = 5.0
highest = lax.Precision.HIGHEST
f32 = jnp.float32
bf16 = jnp.bfloat16
LOG2E = 1.4426950408889634
TERMS = 40
SLAB = 48
DEPTH = 256


def vmem(count):
    return [pl.BlockSpec(memory_space=pltpu.VMEM) for _ in range(count)]


def cost(flops, moved):
    return pl.CostEstimate(flops=int(flops), bytes_accessed=int(moved), transcendentals=0)


def dot_rows(left, right):
    return lax.dot_general(left, right, (((0,), (0,)), ((), ())), preferred_element_type=f32)


def anywhere(count):
    return [pl.BlockSpec(memory_space=pl.ANY) for _ in range(count)]


def fetch(pairs, sems):
    copies = [pltpu.make_async_copy(src, dst, sems.at[i]) for i, (src, dst) in enumerate(pairs)]
    for copy in copies:
        copy.start()
    for copy in copies:
        copy.wait()


def exact(left, right, contract):
    return lax.dot_general(
        left, right, ((contract[:1], contract[1:]), ((), ())), precision=highest,
        preferred_element_type=f32,
    )


def lane_repeat(channels):
    lane = lax.broadcasted_iota(jnp.int32, (channels, 128), 1)
    row = lax.broadcasted_iota(jnp.int32, (channels, 128), 0)
    return jnp.where(lane % channels == row, 1.0, 0.0)


def split(values):
    high = values.astype(bf16)
    return high, (values - high.astype(f32)).astype(bf16)


def centred_embedding(embed, bias):
    width = embed.shape[1]
    embed = embed - jnp.sum(embed, -1, keepdims=True) * (1.0 / width)
    bias = bias - jnp.sum(bias, -1, keepdims=True) * (1.0 / width)
    return embed, bias


def with_tail(body, first, second):
    row = lax.broadcasted_iota(jnp.int32, (16, body.shape[1]), 0)
    tail = jnp.where(row == 0, first, jnp.where(row == 1, second, 0.0))
    return jnp.concatenate([body, tail], 0)


def partial_kernel(seq_count, embed_ref, bias_ref, mod_ref, weight_ref, keep_ref, send_ref):
    seq_index = lax.axis_index("seq")
    core = seq_index % 2
    depth = weight_ref.shape[0]
    half = keep_ref.shape[1]
    embed = embed_ref[...].astype(f32)
    width = embed.shape[1]
    embed_mean = jnp.sum(embed, -1, keepdims=True) * (1.0 / width)
    bias_mean = jnp.sum(bias_ref[...], -1, keepdims=True) * (1.0 / width)
    start = (lax.axis_index("cfg") * seq_count + seq_index) * depth
    base = pl.multiple_of(start // 128 * 128, 128)
    offset = start - base
    window = pl.ds(base, 128)
    scale = 1.0 + mod_ref[1:2, window]
    rows = with_tail(
        (embed_ref[:, window].astype(f32) - embed_mean) * scale,
        (bias_ref[:, window] - bias_mean) * scale,
        mod_ref[0:1, window],
    )
    rows = pltpu.roll(rows, (128 - offset) % 128, 1)[:, :depth]
    high, low = split(rows)
    left = jnp.concatenate([high, low], 0)

    def part(which):
        columns = pl.ds(pl.multiple_of(which * half, 128), half)
        product = jnp.dot(left, weight_ref[:, columns], preferred_element_type=f32)
        return product[:TERMS] + product[SLAB : SLAB + TERMS]

    send_ref[...] = part(1 - core)
    keep_ref[...] = part(core)


def velocity_kernel(
    hidden_ref, mod_ref, weight_ref, shift_ref, key_gain_ref, query_gain_ref, out_ref, small_ref
):
    small_ref[...] = jnp.zeros_like(small_ref)
    small_ref[0:1, 0 : shift_ref.shape[1]] = shift_ref[...]
    small_ref[1:2, :] = key_gain_ref[...]
    small_ref[2:3, :] = query_gain_ref[...]
    values = hidden_ref[...].astype(f32)
    width = values.shape[1]
    centred = values - jnp.sum(values, -1, keepdims=True) * (1.0 / width)
    variance = jnp.sum(centred * centred, -1, keepdims=True) * (1.0 / width)
    normed = centred * lax.rsqrt(variance + epsilon)
    modulated = (normed * (1.0 + mod_ref[1:2, :]) + mod_ref[0:1, :]).astype(bf16)
    out_ref[...] = lax.dot_general(
        weight_ref[...], modulated, (((1,), (1,)), ((), ())), preferred_element_type=f32
    )


def guide_kernel(
    rows,
    table_ref,
    latent_ref,
    step_any,
    slot_any,
    own_any,
    other_any,
    guided_ref,
    next_ref,
    step_ref,
    slot_ref,
    own_ref,
    other_ref,
    sems,
):
    fetch(
        [(step_any, step_ref), (slot_any, slot_ref), (own_any, own_ref), (other_any, other_ref)], sems
    )
    branch = lax.axis_index("cfg")
    own = own_ref[...]
    other = other_ref[...]
    channels, count = own.shape
    group = 128 // channels
    cells = count // rows
    line = lax.broadcasted_iota(jnp.int32, (count // group, count), 0)
    column = lax.broadcasted_iota(jnp.int32, (count // group, count), 1)
    belongs = jnp.where(line == column % cells // group * rows + column // cells, 1.0, 0.0)
    lane = lax.broadcasted_iota(jnp.int32, (count, 128), 1)
    cell = lax.broadcasted_iota(jnp.int32, (count, 128), 0)
    slot = lane // channels == cell % group
    repeat = lane_repeat(channels)
    spread = jnp.where(slot, exact(belongs, latent_ref[...], (0, 0)), 0.0)
    latent = exact(repeat, spread, (1, 1))
    first = branch == 0
    conditional = jnp.where(first, own, other)
    unconditional = jnp.where(first, other, own)
    table = table_ref[...]
    slots = lax.broadcasted_iota(jnp.int32, table.shape, 0) * table.shape[
        1
    ] + lax.broadcasted_iota(jnp.int32, table.shape, 1)
    picked = jnp.where(slots == slot_ref[0], table, 0.0)
    guidance = jnp.sum(jnp.sum(picked, 0, keepdims=True), 1, keepdims=True)
    guided = unconditional + guidance * (conditional - unconditional)

    def sigma(step):
        fraction = 1.0 - jnp.full((1, 1), step, jnp.int32).astype(f32) / STEPS
        return flow_shift * fraction / (1.0 + (flow_shift - 1.0) * fraction)

    change = sigma(step_ref[0] + 1) - sigma(step_ref[0])
    next_ref[...] = latent + change * guided
    guided_ref[...] = exact(belongs, jnp.where(slot, exact(guided, repeat, (0, 0)), 0.0), (1, 0))


def fine_kernel(
    cells,
    taps_ref,
    small_ref,
    embed_ref,
    bias_ref,
    text_ref,
    near_any,
    own_any,
    far_any,
    fine_ref,
    keys_ref,
    keys_t_ref,
    query_ref,
    token_ref,
    text_out_ref,
    near_ref,
    own_ref,
    far_ref,
    sems,
):
    fetch([(near_any, near_ref), (own_any, own_ref), (far_any, far_ref)], sems)
    channels, own_lanes = own_ref.shape
    rows = own_lanes // cells
    lanes = (rows + 2) * cells
    gain = small_ref[1:2, :]
    head = gain.shape[1]
    for h in range(text_ref.shape[1] // head):
        part = text_ref[:, h * head : (h + 1) * head].astype(f32)
        mean = jnp.sum(part * part, -1, keepdims=True) * (1.0 / head)
        text_out_ref[:, h * head : (h + 1) * head] = (
            part * lax.rsqrt(mean + epsilon) * gain
        ).astype(bf16)

    even = lax.axis_index("seq") % 2 == 0
    up = jnp.where(even, far_ref[...], near_ref[...])
    down = jnp.where(even, near_ref[...], far_ref[...])
    extended = jnp.concatenate([up, own_ref[...], down], 1)
    total = extended.shape[1]
    origin = own_lanes - cells
    lane = lax.broadcasted_iota(jnp.int32, (channels, lanes), 1) % cells

    def shifted(down, right):
        start = origin + down * cells + right
        moved = pltpu.roll(extended, (-start) % total, 1)[:, :lanes]
        if right < 0:
            moved = jnp.where(lane == 0, 0.0, moved)
        if right > 0:
            moved = jnp.where(lane == cells - 1, 0.0, moved)
        return moved

    around = {(i, j): shifted(i, j) for i in (-1, 0, 1) for j in (-1, 0, 1)}

    taps = taps_ref[...].T
    same = lax.broadcasted_iota(jnp.int32, (channels, channels), 0) == lax.broadcasted_iota(
        jnp.int32, (channels, channels), 1
    )
    shift = jnp.sum(jnp.where(same, small_ref[0:1, :channels], 0.0), 1, keepdims=True)

    def tap(r, s):
        first = (3 * r + s) * channels
        return taps[first : first + channels, :]

    blocks = {}
    for a in range(2):
        for c in range(2):
            patches, weights = [], []
            for i in (a - 1, a):
                for j in (c - 1, c):
                    merged = None
                    for r in range(3):
                        for s in range(3):
                            if (a + r - 1) // 2 == i and (c + s - 1) // 2 == j:
                                merged = tap(r, s) if merged is None else merged + tap(r, s)
                    patches.append(around[i, j])
                    weights.append(merged)
            stacked = jnp.concatenate(weights, 0).T
            product = jnp.dot(
                stacked, jnp.concatenate(patches, 0), precision=highest, preferred_element_type=f32
            )
            blocks[a, c] = product + shift + around[0, 0]

    embed, bias = centred_embedding(embed_ref[...].astype(f32), bias_ref[...])
    high, low = split(with_tail(embed, bias, jnp.zeros_like(bias)))
    pair = jnp.concatenate([high, low], 0)
    width = embed.shape[1]
    step = min(width, 512)

    def features(tokens):
        count = tokens.shape[1]
        one = jnp.ones((1, count), f32)
        values = with_tail(tokens.astype(f32), one, jnp.zeros_like(one)).astype(bf16)
        double = jnp.concatenate([values, values], 0)
        square = jnp.zeros((1, count), f32)
        for first in range(0, width, step):
            state = dot_rows(pair[:, first : first + step], double)
            square += jnp.sum(state * state, 0, keepdims=True)
        spread = lax.rsqrt(square * (1.0 / width) + epsilon)
        top, rest = split(with_tail(tokens.astype(f32) * spread, spread, one))
        fill = jnp.zeros((DEPTH - 3 * SLAB, count), bf16)
        return jnp.concatenate([top, rest, top, fill], 0)

    for a in range(2):
        for c in range(2):
            turned = features(blocks[a, c].astype(bf16)).T
            for r in range(rows + 2):
                first = (4 * r + 2 * a + c) * cells
                keys_ref[first : first + cells, :] = turned[r * cells : (r + 1) * cells, :]
    keys_t_ref[...] = keys_ref[...].T

    parity = lax.axis_index("cfg")
    tokens = jnp.zeros((channels, 2 * own_lanes), f32)
    cell = lax.broadcasted_iota(jnp.int32, (own_lanes, 2 * own_lanes), 0)
    place = lax.broadcasted_iota(jnp.int32, (own_lanes, 2 * own_lanes), 1)
    group = 128 // channels
    fine_lines = 2 * own_lanes // group
    line = lax.broadcasted_iota(jnp.int32, (fine_lines, own_lanes), 0)
    column = lax.broadcasted_iota(jnp.int32, (fine_lines, own_lanes), 1)
    belongs = jnp.where(line == 2 * column // group, 1.0, 0.0)
    lane128 = lax.broadcasted_iota(jnp.int32, (own_lanes, 128), 1) // channels
    cell128 = lax.broadcasted_iota(jnp.int32, (own_lanes, 128), 0)
    repeat = lane_repeat(channels)
    fine = jnp.zeros((own_lanes, 128), f32)
    for c in range(2):
        mine = jnp.where(parity == 0, blocks[0, c], blocks[1, c])
        mine = pltpu.roll(mine, lanes - cells, 1)[:, :own_lanes]
        fine += jnp.where(lane128 == (2 * cell128 + c) % group, exact(mine, repeat, (0, 0)), 0.0)
        chosen = jnp.where(place == 2 * cell + c, 1.0, 0.0).astype(bf16)
        tokens += jnp.dot(mine.astype(bf16), chosen, preferred_element_type=f32)
    fine_ref[...] = exact(belongs, fine, (1, 0))
    token_ref[...] = tokens.astype(bf16)
    query_ref[...] = features(tokens.astype(bf16)).T


def attend_kernel(
    rows,
    window,
    keys_ref,
    keys_t_ref,
    query_ref,
    small_ref,
    text_ref,
    text_values_ref,
    length_any,
    kept_any,
    other_any,
    out_ref,
    mix_ref,
    value_ref,
    gain_ref,
    length_ref,
    kept_ref,
    other_ref,
    sems,
):
    step = pl.program_id(0)
    seq_index = lax.axis_index("seq")
    head = small_ref.shape[1]
    half = kept_ref.shape[1]
    key_count = keys_ref.shape[0]
    text_count, span = text_ref.shape
    per_step = span // head
    inner = pl.num_programs(0) * span
    low_ok = seq_index > 0
    high_ok = seq_index < lax.axis_size("seq") - 1
    key_row = lax.broadcasted_iota(jnp.int32, (key_count, head), 0)
    allowed = (low_ok | (key_row >= window)) & (high_ok | (key_row < key_count - window))
    text_row = lax.broadcasted_iota(jnp.int32, (text_count, head), 0)
    text_rows = slice(key_count, key_count + text_count)

    @pl.when(step == 0)
    def _():
        fetch([(length_any, length_ref), (kept_any, kept_ref), (other_any, other_ref)], sems)
        text_allowed = text_row < length_ref[0]
        core = seq_index % 2
        mix_ref[...] = jnp.zeros_like(mix_ref)
        for side, part_ref in ((core, kept_ref), (1 - core, other_ref)):
            top, rest = split(part_ref[...])
            where = pl.ds(pl.multiple_of(side * half, 128), half)
            mix_ref[0:TERMS, where] = top
            mix_ref[SLAB : SLAB + TERMS, where] = top
            mix_ref[2 * SLAB : 2 * SLAB + TERMS, where] = rest
        for i in range(per_step):
            value_ref[i, 0:key_count, head : 2 * head] = jnp.where(allowed, 1.0, 0.0).astype(bf16)
            value_ref[i, text_rows, head : 2 * head] = jnp.where(text_allowed, 1.0, 0.0).astype(
                bf16
            )
        same = lax.broadcasted_iota(jnp.int32, (head, head), 0) == lax.broadcasted_iota(
            jnp.int32, (head, head), 1
        )
        column = jnp.sum(jnp.where(same, small_ref[1:2, :], 0.0), 1, keepdims=True)
        gain_ref[...] = jnp.broadcast_to(column, gain_ref.shape)

    text_allowed = text_row < length_ref[0]

    def columns(which):
        return pl.ds(pl.multiple_of(which * inner + step * span, 128), span)

    queries = jnp.dot(query_ref[...], mix_ref[:, columns(0)], preferred_element_type=f32)
    all_keys = dot_rows(mix_ref[:, columns(1)], keys_t_ref[...])
    values = jnp.dot(keys_ref[...], mix_ref[:, columns(2)], preferred_element_type=f32)
    factor = head ** (-0.5) * LOG2E
    tokens = queries.shape[0] // rows
    for i in range(per_step):
        mine = slice(i * head, (i + 1) * head)
        query = queries[:, mine]
        mean = jnp.sum(query * query, -1, keepdims=True) * (1.0 / head)
        query = (query * lax.rsqrt(mean + epsilon) * small_ref[2:3, :]).astype(bf16)
        keys = all_keys[mine]
        mean = jnp.sum(keys * keys, 0, keepdims=True) * (1.0 / head)
        keys = (keys * lax.rsqrt(mean + epsilon) * gain_ref[:, 0:1]).astype(bf16)
        value_ref[i, 0:key_count, 0:head] = jnp.where(allowed, values[:, mine], 0.0).astype(bf16)
        value_ref[i, text_rows, 0:head] = jnp.where(
            text_allowed, text_values_ref[:, mine].astype(f32), 0.0
        ).astype(bf16)
        for r in range(rows):
            part = query[r * tokens : (r + 1) * tokens]
            near = slice(r * window, (r + 3) * window)
            scores = jnp.dot(part, keys[:, near], preferred_element_type=f32)
            text_scores = lax.dot_general(
                part, text_ref[:, mine], (((1,), (1,)), ((), ())), preferred_element_type=f32
            )
            mixed = jnp.dot(
                jnp.exp2(scores * factor).astype(bf16),
                value_ref[i, near, :],
                preferred_element_type=f32,
            ) + jnp.dot(
                jnp.exp2(text_scores * factor).astype(bf16),
                value_ref[i, text_rows, :],
                preferred_element_type=f32,
            )
            out_ref[r * tokens : (r + 1) * tokens, mine] = (mixed[:, :head] / mixed[:, head:]).astype(
                bf16
            )


def output_kernel(
    levels,
    last,
    attended_ref,
    token_ref,
    embed_ref,
    bias_ref,
    mod_ref,
    own_first_ref,
    own_second_ref,
    other_first_ref,
    other_second_ref,
    *rest,
):
    if last:
        ready_ref, out_any, block_ref, sems = rest
    else:
        (block_ref,) = rest
    count, piece, _ = own_first_ref.shape
    seq_index = lax.axis_index("seq")
    core = seq_index % 2
    low = len(levels) - 3
    seq_chips = lax.axis_size("seq") // 2
    attended = attended_ref[...]
    tokens = token_ref[...]
    lanes = 2 * piece
    sides = ((own_first_ref, other_first_ref), (own_second_ref, other_second_ref))
    group = 2
    copies = []

    def place(top, index, upper):
        first, second = (index >> low & 1, upper) if top == 0 else (upper, index >> low & 1)
        flip = second + (top << (levels[-1][1] - 1))
        for j in range(low):
            flip = flip + ((index >> j & 1) << (levels[2 + j][1] - 1))
        chip = (lax.axis_index("cfg") ^ first) * seq_chips + (seq_index // 2 ^ flip)
        return pl.ds(pl.multiple_of(chip * lanes, lanes), lanes)

    def send(source, slot, where, sem):
        copy = pltpu.make_async_copy(source.at[slot], out_any.at[:, where], sems.at[sem])
        copy.start()
        copies.append(copy)

    if last:
        for top in range(2):
            for index in range(count):
                slot = top * count + index
                send(ready_ref, slot, place(top, index, 0), slot)
    for top, (own_ref, other_ref) in enumerate(sides):
        for start in range(0, count, group):
            blocks = []
            for index in range(start, start + group):
                blocks += [own_ref[index], other_ref[index]]
            product = lax.dot_general(
                attended,
                jnp.concatenate(blocks, 0),
                (((1,), (1,)), ((), ())),
                preferred_element_type=f32,
            )
            for i in range(group):
                index = start + i
                where = place(top, index, last)
                block = pltpu.roll(product[:, i * lanes : (i + 1) * lanes], core * piece, 1)
                state = dot_rows(tokens, embed_ref[:, where]) + bias_ref[:, where]
                slot = top * count + index
                block_ref[slot] = (state + mod_ref[2:3, where] * block).astype(bf16)
                if last:
                    send(block_ref, slot, where, 2 * count + slot)
    for copy in copies:
        copy.wait()


def per_device(
    coarse_hidden,
    coarse_modulation,
    final_weight,
    coarse_latent,
    step_index,
    guide_index,
    guide_scales,
    upsample_weight,
    upsample_bias,
    embed_weight,
    embed_bias,
    fine_modulation,
    project_weight,
    query_gain,
    key_gain,
    text_keys,
    text_values,
    text_length,
    output_weight,
):
    rows = coarse_hidden.shape[1]
    cells = coarse_hidden.shape[2]
    width = coarse_hidden.shape[3]
    channels = final_weight.shape[1]
    head = query_gain.shape[0]
    inner = project_weight.shape[1] // 3
    cfg_count = lax.axis_size("cfg")
    seq_count = lax.axis_size("seq")
    seq_index = lax.axis_index("seq")
    seq_bits = seq_count.bit_length() - 1
    assert seq_count == 1 << seq_bits and cfg_count == 2 and rows >= 2 and seq_bits >= 3
    own = rows * cells
    fine_tokens = 2 * own
    key_count = (rows + 2) * 4 * cells
    text_count = text_keys.shape[0]
    bias_row = embed_bias.reshape(1, width)

    def swap(value, *stages):
        size = cfg_count * seq_count
        flip = 0
        for axis, bit in stages:
            flip |= seq_count if axis == "cfg" else 1 << bit
        return lax.ppermute(value, ("cfg", "seq"), [(i, i ^ flip) for i in range(size)])

    across = ("seq", 0)
    levels = [("cfg", 0)] + [("seq", bit) for bit in range(1, seq_bits)]

    half = 3 * inner // 2
    kept, sent = pl.pallas_call(
        functools.partial(partial_kernel, seq_count),
        out_shape=(jax.ShapeDtypeStruct((TERMS, half), f32),) * 2,
        in_specs=vmem(4),
        out_specs=tuple(vmem(2)),
        cost_estimate=cost(2e9, 1e6),
        name="partial_mix",
    )(embed_weight, bias_row, fine_modulation, project_weight)
    met = swap(sent, across)

    velocity, small = pl.pallas_call(
        velocity_kernel,
        out_shape=(
            jax.ShapeDtypeStruct((channels, own), f32),
            jax.ShapeDtypeStruct((8, head), f32),
        ),
        in_specs=vmem(6),
        out_specs=tuple(vmem(2)),
        cost_estimate=cost(2e9, 1e6),
        name="velocity",
        compiler_params=pltpu.CompilerParams(vmem_limit_bytes=6 << 20),
    )(
        coarse_hidden.reshape(own, width),
        coarse_modulation[0],
        final_weight.T,
        upsample_bias.reshape(1, channels),
        key_gain.reshape(1, head),
        query_gain.reshape(1, head),
    )
    partner = swap(velocity, ("cfg", 0))

    held = output_weight.T[None]

    def doubled(block, stage):
        return jnp.concatenate([block, swap(block, stage)], 0)

    first, second = levels[0], levels[1]
    total = kept + met
    rounded = total.astype(bf16)
    for stage in levels[2:]:
        held = doubled(held, stage)
    total = (
        total
        + swap(rounded, first).astype(f32)
        + swap(rounded, second).astype(f32)
        + swap(rounded, first, second).astype(f32)
    )

    lines = own * channels // 128
    latent = coarse_latent.reshape(rows, lines // rows, 128).transpose(1, 0, 2).reshape(lines, 128)
    guided, stepped = pl.pallas_call(
        functools.partial(guide_kernel, rows),
        out_shape=(
            jax.ShapeDtypeStruct((lines, 128), f32),
            jax.ShapeDtypeStruct((channels, own), f32),
        ),
        in_specs=vmem(2) + anywhere(4),
        out_specs=tuple(vmem(2)),
        scratch_shapes=[pltpu.SMEM((1,), jnp.int32)] * 2
        + [pltpu.VMEM((channels, own), f32)] * 2
        + [pltpu.SemaphoreType.DMA((4,))],
        cost_estimate=cost(1e9, 1e5),
        name="guide",
        compiler_params=pltpu.CompilerParams(vmem_limit_bytes=2 << 20),
    )(
        guide_scales.reshape(-1, 128),
        latent,
        step_index,
        guide_index,
        velocity,
        partner,
    )

    near_rows = swap(stepped, across)
    ahead = [(i, i + 1) for i in range(1, seq_count - 1, 2)]
    behind = [(target, source) for source, target in ahead]
    far_rows = lax.ppermute(stepped, "seq", ahead + behind)

    fine, keys, keys_t, query, tokens, text_normed = pl.pallas_call(
        functools.partial(fine_kernel, cells),
        out_shape=(
            jax.ShapeDtypeStruct((2 * lines, 128), f32),
            jax.ShapeDtypeStruct((key_count, DEPTH), bf16),
            jax.ShapeDtypeStruct((DEPTH, key_count), bf16),
            jax.ShapeDtypeStruct((fine_tokens, DEPTH), bf16),
            jax.ShapeDtypeStruct((channels, fine_tokens), bf16),
            jax.ShapeDtypeStruct(text_keys.shape, bf16),
        ),
        in_specs=vmem(5) + anywhere(3),
        out_specs=tuple(vmem(6)),
        scratch_shapes=[pltpu.VMEM((channels, own), f32)] * 3 + [pltpu.SemaphoreType.DMA((3,))],
        cost_estimate=cost(4e9, 4e6),
        name="fine_features",
        compiler_params=pltpu.CompilerParams(vmem_limit_bytes=20 << 20),
    )(
        upsample_weight.T,
        small,
        embed_weight,
        bias_row,
        text_keys,
        near_rows,
        stepped,
        far_rows,
    )

    for stage in levels[2:]:
        moved = swap(total.astype(bf16), stage)
        total = total + moved.astype(f32)
    others = swap(total, across)

    middle = held.shape[0] // 2
    own_first, own_second = held[:middle], held[middle:]
    own_first = doubled(own_first, first)
    own_second = doubled(own_second, second)
    far_first = swap(own_first, second)
    far_second = swap(own_second, first)
    near_pieces = (own_first, own_second, swap(own_first, across), swap(own_second, across))
    far_pieces = (far_first, far_second, swap(far_first, across), swap(far_second, across))

    whole = pl.BlockSpec(memory_space=pltpu.VMEM)
    free = pl.BlockSpec(memory_space=pl.ANY)
    span = 2 * head
    per_step = pl.BlockSpec((text_count, span), lambda h: (0, h))
    attended = pl.pallas_call(
        functools.partial(attend_kernel, rows, 4 * cells),
        grid=(inner // span,),
        out_shape=jax.ShapeDtypeStruct((fine_tokens, inner), bf16),
        in_specs=[whole] * 4 + [per_step, per_step, free, free, free],
        out_specs=pl.BlockSpec((fine_tokens, span), lambda h: (0, h)),
        scratch_shapes=[
            pltpu.VMEM((DEPTH, 3 * inner), bf16),
            pltpu.VMEM((2, key_count + text_count, 2 * head), bf16),
            pltpu.VMEM((head, 128), f32),
            pltpu.SMEM((1,), jnp.int32),
            pltpu.VMEM((TERMS, half), f32),
            pltpu.VMEM((TERMS, half), f32),
            pltpu.SemaphoreType.DMA((3,)),
        ],
        cost_estimate=cost(8e9, 4e6),
        name="attend",
        compiler_params=pltpu.CompilerParams(vmem_limit_bytes=24 << 20),
    )(
        keys,
        keys_t,
        query,
        small,
        text_normed,
        text_values,
        text_length,
        total,
        others,
    )

    piece = output_weight.shape[1]
    count = own_first.shape[0]
    if 2 * piece == 128:

        block_shape = (2 * count, fine_tokens, 128)

        def output(last, pieces, *before):
            if last:
                out_shape = jax.ShapeDtypeStruct((fine_tokens, width), bf16)
                scratch = [pltpu.VMEM(block_shape, bf16), pltpu.SemaphoreType.DMA((4 * count,))]
            else:
                out_shape = jax.ShapeDtypeStruct(block_shape, bf16)
                scratch = []
            return pl.pallas_call(
                functools.partial(output_kernel, tuple(levels), last),
                out_shape=out_shape,
                in_specs=[whole] * (9 + len(before)),
                out_specs=free if last else whole,
                scratch_shapes=scratch,
                cost_estimate=cost(1e9, 3e6),
                compiler_params=pltpu.CompilerParams(vmem_limit_bytes=16 << 20),
            )(attended, tokens, embed_weight, bias_row, fine_modulation, *pieces, *before)

        near = output(0, near_pieces)
        hidden = output(1, far_pieces, near)
    else:
        low = len(levels) - 3
        chip = jnp.arange(4 * count, dtype=jnp.int32)
        seq_chips = seq_count // 2
        apart = chip // seq_chips ^ lax.axis_index("cfg")
        flip = chip % seq_chips ^ seq_index // 2
        side = flip & 1
        top = flip >> (levels[-1][1] - 1) & 1
        position = top * count + (jnp.where(top == 0, apart, side) << low)
        position = position + jnp.where(top == 0, side, apart) * (2 * count)
        for j in range(low):
            position = position + ((flip >> (levels[2 + j][1] - 1) & 1) << j)
        mine = jnp.take(jnp.concatenate(near_pieces[:2] + far_pieces[:2], 0), position, axis=0)
        theirs = jnp.take(jnp.concatenate(near_pieces[2:] + far_pieces[2:], 0), position, axis=0)
        even = seq_index % 2 == 0
        both = jnp.stack([jnp.where(even, mine, theirs), jnp.where(even, theirs, mine)], 1)
        product = lax.dot_general(
            attended,
            both.reshape(width, inner),
            (((1,), (1,)), ((), ())),
            preferred_element_type=f32,
        )
        state = dot_rows(tokens, embed_weight) + bias_row
        hidden = (state + fine_modulation[2:3] * product).astype(bf16)

    guided = guided.reshape(lines // rows, rows, 128).transpose(1, 0, 2)
    return (
        guided.reshape(rows, cells * channels),
        fine.reshape(rows, 1, 2 * cells * channels),
        hidden.reshape(rows, 1, 2 * cells, width),
    )


def solution(mesh):
    placed = (
        P("cfg", "seq", None, None),
        P("cfg", None, None),
        P(),
        P("seq", None),
        P(),
        P(),
        P(),
        P(),
        P(),
        P(),
        P(),
        P(),
        P(("cfg", "seq"), None),
        P(),
        P(),
        P(),
        P(),
        P(),
        P(None, ("cfg", "seq")),
    )
    return jax.shard_map(
        per_device,
        mesh=mesh,
        in_specs=placed,
        out_specs=(P("seq", None), P("seq", "cfg", None), P("seq", "cfg", None, None)),
        check_vma=False,
    )
```
